32 devices in a mesh: site: 2 (over core), rows: 2 (over x), cols: 8 (over z, y).
Axes of the slice: x: 2, y: 2, z: 4, core: 2. Of those that a mesh axis runs over, the one named last changes fastest.
Arguments:
- tracer: float32 [128, 256, 128], P(('site', 'rows'), 'cols'), parts along dimension 0, may hold values from 0.5 to 2
- flow_y: float32 [128, 256, 128], P(('site', 'rows'), 'cols'), parts along dimension 0, may hold values from -0.3 to 0.3
- flow_x: float32 [128, 256, 128], P(('site', 'rows'), 'cols'), parts along dimension 0, may hold values from -0.3 to 0.3
Outputs:
- scaled_field: float32 [128, 256, 128], P(('site', 'rows'), 'cols'), parts along dimension 0
- tracer_end: float32 [128, 256, 128], P(('site', 'rows'), 'cols'), parts along dimension 0
The draws below stay inside these ranges and needn't reach their ends.
There are 2 independent parts, one for each index of `site`. The reference program is written for one: setup_inputs(seed, part) draws one part's arguments, and reference() takes and returns one part's arrays. A program takes and returns all parts, laid end to end along the dimension named above; each array names one. Nothing has to cross between parts.
All inputs are finite; a program needn't handle non-finite values.
Results may differ from the reference program's by a relative error of at most 0.00002.
Values sent between devices are 32-bit elements; how exact they have to be, the bound alone decides.
A program may use at most 64 MiB of HBM per device.

```python
import jax
import jax.numpy as jnp
from jax import lax

GRID_Y = 64
GRID_X = 256
SPECIES = 128
STEPS = 6


def block_levels(rng, shape, cuts, low, top_value):
    def one(dim, parts):
        heights = jax.random.uniform(jax.random.fold_in(jax.random.fold_in(rng, 6), dim), (parts,), jnp.float32, low / len(cuts), top_value / len(cuts))
        return jnp.repeat(jnp.exp(heights), shape[dim] // parts).reshape((-1,) + (1,) * (len(shape) - dim - 1))

    factor_of = one(*cuts[0])
    for cut in cuts[1:]:
        factor_of = factor_of * one(*cut)
    return factor_of


def setup_inputs(seed: int = 0, part: int = 0) -> dict:
    streams_of = jax.random.split(jax.random.key(seed), 4)
    part_splits = jax.random.split(jax.random.fold_in(streams_of[3], part), 4)
    return {
        "tracer": jnp.clip(0.5 + 1.5 * jax.random.uniform(part_splits[0], (GRID_Y, GRID_X, SPECIES), jnp.float32) ** block_levels(part_splits[0], (GRID_Y, GRID_X, SPECIES), ((0, 2), (1, 8)), -0.2, 0.2), 0.5, 2.0),
        "flow_y": jnp.clip(jax.random.uniform(part_splits[1], (GRID_Y, GRID_X, SPECIES), jnp.float32, -0.3, 0.3) * block_levels(part_splits[1], (GRID_Y, GRID_X, SPECIES), ((0, 2), (1, 8)), -0.4, 0.0), -0.3, 0.3),
        "flow_x": jnp.clip(jax.random.uniform(part_splits[2], (GRID_Y, GRID_X, SPECIES), jnp.float32, -0.3, 0.3) * block_levels(part_splits[2], (GRID_Y, GRID_X, SPECIES), ((0, 2), (1, 8)), -0.4, 0.0), -0.3, 0.3),
    }


def strip_edges(values, dims):
    for dim in dims:
        values = lax.slice_in_dim(values, 1, values.shape[dim] - 1, axis=dim)
    return values

def neighbour(values, dim, start, dims):
    others = [other for other in dims if other != dim]
    values = strip_edges(values, others)
    return lax.slice_in_dim(values, start, start + values.shape[dim] - 2, axis=dim)

def one_step(padded, flow_y, flow_x):
    middle = strip_edges(padded, (0, 1))
    lower = [neighbour(padded, dim, 0, (0, 1)) for dim in (0, 1)]
    upper = [neighbour(padded, dim, 2, (0, 1)) for dim in (0, 1)]
    slopes = [above - below for above, below in zip(upper, lower)]
    smooth_rate = 0.05
    spread = lower[0] + upper[0] + lower[1] + upper[1] - 4.0 * middle
    return middle - flow_y * slopes[0] - flow_x * slopes[1] + smooth_rate * spread

def reference(tracer, flow_y, flow_x):
    for step in range(STEPS):
        tracer = one_step(jnp.pad(tracer, ((1, 1), (1, 1), (0, 0)), mode='constant'), flow_y, flow_x)
    line_mean = lax.optimization_barrier(jnp.mean(tracer, axis=1, keepdims=True))
    centred = tracer - line_mean
    line_variance = lax.optimization_barrier(jnp.mean(centred * centred, axis=1, keepdims=True))
    scaled_field = centred * lax.rsqrt(line_variance + 0.0001)
    return (scaled_field, tracer)
```

```python
import functools

import jax
import jax.numpy as jnp
from jax import lax
from jax.experimental import pallas as pl
from jax.experimental.pallas import tpu as pltpu
from jax.sharding import PartitionSpec as P

MESH = pl.DeviceIdType.MESH
STEPS, DEPTH = 6, 3
PHASES = STEPS // DEPTH
PAD = 8
HALF = PAD // 2
CUTS = (8,)
SIDES = tuple((dy, dx) for dy in (-1, 1, 0) for dx in (-1, 1, 0) if (dy, dx) != (0, 0))
CORNERS = tuple(side for side in SIDES if side[0] and side[1])


def radii(cols):
    out, r = [], 1
    while r < cols - 1:
        out.append(r)
        r *= 2
    return out


def kernel(rows, cols, by, bx, cuts, t_hbm, fy_hbm, fx_hbm, final, moments,
           main, halo, f, fh, weight, stats, gathered,
           load_sem, col_send, col_recv, row_send, row_recv, corner_send, corner_recv,
           stat_send, stat_recv, tokens):
    row, col = lax.axis_index("rows"), lax.axis_index("cols")
    top = DEPTH
    tall = by + 2 * top
    chunks = len(cuts) - 1
    odd = lax.rem(row, 2) == 1

    def exists(dy, dx):
        ok = None
        for step, here, count in ((dy, row, rows), (dx, col, cols)):
            if step:
                inside = (here > 0) if step < 0 else (here < count - 1)
                ok = inside if ok is None else jnp.logical_and(ok, inside)
        return ok

    def at(v, n):
        return jnp.where(odd, top + v, top + by - v - n)

    barrier = pltpu.get_barrier_semaphore()
    for dy, dx in SIDES:
        if dy and dx:
            continue

        @pl.when(exists(dy, dx))
        def _():
            pl.semaphore_signal(barrier, inc=1, device_id={"rows": row + dy, "cols": col + dx},
                                device_id_type=MESH)

    loads = [
        pltpu.make_async_copy(t_hbm, main.at[0, pl.ds(top, by)], load_sem.at[0]),
        pltpu.make_async_copy(fy_hbm, f.at[0, pl.ds(top, by)], load_sem.at[1]),
        pltpu.make_async_copy(fx_hbm, f.at[1, pl.ds(top, by)], load_sem.at[2]),
    ]
    for load in loads:
        load.start()

    for dy in (-1, 1):
        line = top - 1 if dy < 0 else top + by

        @pl.when(jnp.logical_not(exists(dy, 0)))
        def _():
            for s in range(STEPS):
                main[s, line] = jnp.zeros((bx, 128), jnp.float32)
                halo[s, line] = jnp.zeros((PAD, 128), jnp.float32)
    for dx in (-1, 1):
        strip = pl.ds(HALF, HALF) if dx < 0 else pl.ds(0, HALF)

        @pl.when(jnp.logical_not(exists(0, dx)))
        def _():
            for p in range(PHASES):
                halo[p * DEPTH, :, strip] = jnp.zeros((tall, HALF, 128), jnp.float32)

    def one(n, count):
        return (n + count - 1) // count

    def on_both(r):
        return jnp.where(col >= r, 1, 0) + jnp.where(col < cols - r, 1, 0)

    upright = one(row, rows) + one(rows - 1 - row, rows)
    across = on_both(1)

    for load in loads:
        load.wait()

    @pl.loop(0, by // 4)
    def _(i):
        lines = pl.ds(i * 4, 4)
        for d in range(2):
            flow = f[d, pl.ds(top + i * 4, 4)]
            weight[2 * d, lines] = 0.05 - flow
            weight[2 * d + 1, lines] = 0.05 + flow
    pl.semaphore_wait(barrier, across + upright)

    spread_to = radii(cols)

    def send_token(i):
        if i < len(spread_to):
            r = spread_to[i]
            for sign in (-1, 1):
                @pl.when((col >= r) if sign < 0 else (col < cols - r))
                def _():
                    pl.semaphore_signal(tokens.at[i], inc=1, device_id={"cols": col + sign * r},
                                        device_id_type=MESH)

    def take_token(i):
        if i < len(spread_to):
            pl.semaphore_wait(tokens.at[i], on_both(spread_to[i]))

    def remote(src, dst, send, recv, dy, dx):
        return pltpu.make_async_remote_copy(
            src_ref=src, dst_ref=dst, send_sem=send, recv_sem=recv,
            device_id={"rows": row + dy, "cols": col + dx}, device_id_type=MESH)

    def cols_of(dx, depth):
        if dx > 0:
            return pl.ds(bx - depth, depth), pl.ds(PAD - depth, depth)
        return pl.ds(0, depth), pl.ds(0, depth)

    def rows_of(dy, depth):
        if dy > 0:
            return pl.ds(top + by - depth, depth), pl.ds(top - depth, depth)
        return pl.ds(top, depth), pl.ds(top + by, depth)

    def reach(p, c):
        if c < 0:
            return 0
        return by if c == chunks - 1 else min(by, cuts[c + 1] + STEPS - 1 - p * DEPTH)

    def column_copies(p, c):
        v, n = reach(p, c - 1), reach(p, c) - reach(p, c - 1)
        out = []
        if not n:
            return out
        lines = pl.ds(at(v, n), n)
        for i, dx in enumerate((-1, 1)):
            xs, xd = cols_of(dx, DEPTH)
            mine = [remote(main.at[p * DEPTH, lines, xs], halo.at[p * DEPTH, lines, xd],
                           col_send.at[p, c, i, 0], col_recv.at[p, c, i, 0], 0, dx)]
            if p == 0:
                xs, xd = cols_of(dx, DEPTH - 1)
                mine.append(remote(f.at[:, lines, xs], fh.at[:, lines, xd],
                                   col_send.at[p, c, i, 1], col_recv.at[p, c, i, 1], 0, dx))
            out.append((exists(0, dx), exists(0, -dx), mine))
        return out

    def border_copies(p, first, corners):
        out = []
        for i, dy in enumerate((-1, 1)):
            here = odd if (dy < 0) == first else jnp.logical_not(odd)
            there = odd if (dy > 0) == first else jnp.logical_not(odd)
            ys, yd = rows_of(dy, DEPTH)
            mine = [remote(main.at[p * DEPTH, ys], main.at[p * DEPTH, yd],
                           row_send.at[p, i, 0], row_recv.at[p, i, 0], dy, 0)]
            if p == 0:
                ys, yd = rows_of(dy, DEPTH - 1)
                mine.append(remote(f.at[:, ys], f.at[:, yd],
                                   row_send.at[p, i, 1], row_recv.at[p, i, 1], dy, 0))
            if not corners:
                out.append((jnp.logical_and(here, exists(dy, 0)), jnp.logical_and(there, exists(-dy, 0)), mine))
                continue
            for j, dx in enumerate((-1, 1)):
                (ys, yd), (xs, xd) = rows_of(dy, DEPTH - 1), cols_of(dx, DEPTH - 1)
                mine = [remote(main.at[p * DEPTH, ys, xs], halo.at[p * DEPTH, yd, xd],
                               corner_send.at[p, i, j, 0], corner_recv.at[p, i, j, 0], dy, dx)]
                if p == 0 and DEPTH > 2:
                    (ys, yd), (xs, xd) = rows_of(dy, DEPTH - 2), cols_of(dx, DEPTH - 2)
                    mine.append(remote(f.at[:, ys, xs], fh.at[:, yd, xd],
                                       corner_send.at[p, i, j, 1], corner_recv.at[p, i, j, 1], dy, dx))
                out.append((jnp.logical_and(here, exists(dy, dx)),
                            jnp.logical_and(there, exists(-dy, -dx)), mine))
        return out

    def corner_copies(p, c):
        out = []
        if c == 0:
            out = border_copies(p, True, True)
        if c == chunks - 1 and rows > 2:
            out = out + border_copies(p, False, True)
        return out

    def side_copies(p, c):
        out = column_copies(p, c)
        if c == 0:
            out = out + border_copies(p, True, False)
        if c == chunks - 1 and rows > 2:
            out = out + border_copies(p, False, False)
        return out

    def exchange(p, c):
        return corner_copies(p, c) + side_copies(p, c)

    def start(jobs):
        for here, _, copies in jobs:
            @pl.when(here)
            def _():
                for copy in copies:
                    copy.start()

    def finish(jobs):
        for _, there, copies in jobs:
            @pl.when(there)
            def _():
                for copy in copies:
                    copy.wait_recv()

    def drain(jobs):
        for here, _, copies in jobs:
            @pl.when(here)
            def _():
                for copy in copies:
                    copy.wait_send()

    column = lax.broadcasted_iota(jnp.int32, (1, PAD, 128), 1)
    keep = jnp.logical_and(
        jnp.logical_or(column < HALF, jnp.broadcast_to(col > 0, column.shape)),
        jnp.logical_or(column >= HALF, jnp.broadcast_to(col < cols - 1, column.shape)))

    def mix(c, above, below, right, left, fy, fx):
        spread = (above + below) + (right + left)
        return (0.8 * c + 0.05 * spread) - fy * (above - below) - fx * (right - left)

    def new_main(s, y, k, beyond=False):
        c = main[s, pl.ds(y, k)]
        wide = jnp.concatenate([c, halo[s, pl.ds(y, k)]], axis=1)
        right, left = pltpu.roll(wide, bx + PAD - 1, 1)[:, :bx], pltpu.roll(wide, 1, 1)[:, :bx]
        above, below = main[s, pl.ds(y + 1, k)], main[s, pl.ds(y - 1, k)]
        if beyond:
            return mix(c, above, below, right, left, f[0, pl.ds(y, k)], f[1, pl.ds(y, k)])
        up, down, ahead, back = (weight[i, pl.ds(y - top, k)] for i in range(4))
        return ((0.8 * c + up * above) + down * below) + (ahead * right + back * left)

    def new_halo(s, y, k):
        c = halo[s, pl.ds(y, k)]
        wide = jnp.concatenate([main[s, pl.ds(y, k), pl.ds(bx - PAD, PAD)], c,
                                main[s, pl.ds(y, k), pl.ds(0, PAD)]], axis=1)
        right = pltpu.roll(wide, 3 * PAD - 1, 1)[:, PAD:2 * PAD]
        left = pltpu.roll(wide, 1, 1)[:, PAD:2 * PAD]
        new = mix(c, halo[s, pl.ds(y + 1, k)], halo[s, pl.ds(y - 1, k)], right, left,
                  fh[0, pl.ds(y, k)], fh[1, pl.ds(y, k)])
        return jnp.where(keep, new, 0.0)

    def over(v, n, k, do):
        if n <= 0:
            return
        y = at(v, n)
        whole = n // k
        if whole > 1:
            @pl.loop(0, whole)
            def _(i):
                do(y + i * k, k)
        elif whole:
            do(y, k)
        if n % k:
            do(y + whole * k, n % k)

    def write_main(s, beyond=False):
        def do(y, k):
            main[s, pl.ds(y, k)] = new_main(s - 1, y, k, beyond)
        return do

    def write_halo(s):
        def do(y, k):
            halo[s, pl.ds(y, k)] = new_halo(s - 1, y, k)
        return do

    def advance(p, c):
        for i in range(1, DEPTH + 1):
            s = p * DEPTH + i
            ahead = STEPS - s
            low = 0 if c == 0 else min(by, cuts[c] + ahead)
            high = by if c == chunks - 1 else min(by, cuts[c + 1] + ahead)
            if s == STEPS:
                break
            over(low, high - low, 8, write_main(s))
            if i < DEPTH:
                low = low - 1 if c else 0
                high = high if c == chunks - 1 else high - 1
                over(low, high - low, 16, write_halo(s))
                margin = DEPTH - i
                for first in (True, False):
                    if c != (0 if first else chunks - 1) or not first and rows <= 2:
                        continue
                    for dy in (-1, 1):
                        here = odd if (dy < 0) == first else jnp.logical_not(odd)

                        @pl.when(jnp.logical_and(here, exists(dy, 0)))
                        def _():
                            y = top - margin if dy < 0 else top + by
                            write_main(s, True)(y, margin)
                            write_halo(s)(y, margin)
        return low, high

    def share(c, to, sender):
        n = cuts[c + 1] - cuts[c]
        lines = pl.ds(pl.multiple_of(at(cuts[c], n) - top, 8), n)
        return pltpu.make_async_remote_copy(
            src_ref=stats.at[:, lines], dst_ref=gathered.at[sender, :, lines],
            send_sem=stat_send.at[c, to], recv_sem=stat_recv.at[c, sender],
            device_id={"cols": to}, device_id_type=MESH)

    def each_peer(do):
        if cols <= 8:
            for k in range(cols):
                @pl.when(col != k)
                def _():
                    do(k)
        else:
            @pl.loop(0, cols)
            def _(k):
                @pl.when(col != k)
                def _():
                    do(k)

    def last_step(v, n):
        y = at(v, n)

        @pl.loop(0, n // 8)
        def _(i):
            new = new_main(STEPS - 1, y + i * 8, 8)
            out = pl.ds(pl.multiple_of(y - top + i * 8, 8), 8)
            final[out] = new
            mean = jnp.sum(new, axis=1) / bx
            off = new - mean[:, None, :]
            second = jnp.sum(off * off, axis=1)
            stats[0, out] = mean
            stats[1, out] = second
            gathered[col, 0, out] = mean
            gathered[col, 1, out] = second

    def combine(c):
        n = cuts[c + 1] - cuts[c]
        y = at(cuts[c], n) - top

        @pl.loop(0, n // 8)
        def _(i):
            lines = pl.ds(pl.multiple_of(y + i * 8, 8), 8)
            means = [gathered[k, 0, lines] for k in range(cols)]
            mean = sum(means[1:], means[0]) / cols
            parts = [gathered[k, 1, lines] + bx * ((means[k] - mean) * (means[k] - mean)) for k in range(cols)]
            spread = sum(parts[1:], parts[0])
            moments[0, lines] = mean
            moments[1, lines] = lax.rsqrt(spread / (bx * cols) + 0.0001)

    send_token(0)
    for c in range(chunks):
        start(side_copies(0, c))
    known = 0

    def learn():
        take_token(known)
        send_token(known + 1)
        return known + 1

    if spread_to:
        known = learn()
    for c in range(chunks):
        start(corner_copies(0, c))
    while known < len(spread_to) - 1:
        known = learn()
    for p in range(PHASES):
        for c in range(chunks):
            finish(exchange(p, c))
            low, high = advance(p, c)
            if p + 1 < PHASES:
                start(exchange(p + 1, c))
            else:
                last_step(low, high - low)
                while known < len(spread_to):
                    known = learn()
                each_peer(lambda k: share(c, k, col).start())
    for c in range(chunks):
        each_peer(lambda k: share(c, k, k).wait_recv())
        combine(c)
    for c in range(chunks):
        for p in range(PHASES):
            drain(exchange(p, c))
        each_peer(lambda k: share(c, k, col).wait_send())


def scale_kernel(end, lines, scaled_out, end_out, scaled, sem):
    parts = 4
    g = end.shape[0] // parts
    whole = pltpu.make_async_copy(end, end_out, sem.at[parts])
    stores = [whole]
    for i in range(parts):
        part = pl.ds(i * g, g)
        scaled[part] = (end[part] - lines[0, part][:, None, :]) * lines[1, part][:, None, :]
        store = pltpu.make_async_copy(scaled.at[part], scaled_out.at[part], sem.at[i])
        store.start()
        stores.append(store)
        if i == 0:
            whole.start()
    for store in stores:
        store.wait()


def shards(rows, cols, tracer, flow_y, flow_x):
    by, bx, species = tracer.shape
    cuts = (0,) + tuple(cut for cut in CUTS if cut < by) + (by,)
    chunks = len(cuts) - 1
    tall = by + 2 * DEPTH
    block = jax.ShapeDtypeStruct(tracer.shape, jnp.float32)
    hbm = pl.BlockSpec(memory_space=pl.ANY)
    dma = pltpu.SemaphoreType.DMA
    end, lines = pl.pallas_call(
        functools.partial(kernel, rows, cols, by, bx, cuts),
        out_shape=(pltpu.VMEM(tracer.shape, jnp.float32), pltpu.VMEM((2, by, species), jnp.float32)),
        in_specs=[pl.BlockSpec(memory_space=pltpu.HBM)] * 3,
        out_specs=(pl.BlockSpec(memory_space=pltpu.VMEM),) * 2,
        scratch_shapes=[
            pltpu.VMEM((STEPS, tall, bx, species), jnp.float32),
            pltpu.VMEM((STEPS, tall, PAD, species), jnp.float32),
            pltpu.VMEM((2, tall, bx, species), jnp.float32),
            pltpu.VMEM((2, tall, PAD, species), jnp.float32),
            pltpu.VMEM((4, by, bx, species), jnp.float32),
            pltpu.VMEM((2, by, species), jnp.float32),
            pltpu.VMEM((cols, 2, by, species), jnp.float32),
            dma((3,)),
            dma((PHASES, chunks, 2, 2)), dma((PHASES, chunks, 2, 2)),
            dma((PHASES, 2, 2)), dma((PHASES, 2, 2)),
            dma((PHASES, 2, 2, 2)), dma((PHASES, 2, 2, 2)),
            dma((chunks, cols)), dma((chunks, cols)),
            pltpu.SemaphoreType.REGULAR((max(1, len(radii(cols))),)),
        ],
        compiler_params=pltpu.CompilerParams(
            collective_id=0, has_side_effects=True, vmem_limit_bytes=67043328 - 1024 * 1024),
    )(tracer, flow_y, flow_x)
    return pl.pallas_call(
        scale_kernel,
        out_shape=(block, block),
        in_specs=[pl.BlockSpec(memory_space=pltpu.VMEM)] * 2,
        out_specs=(hbm, hbm),
        scratch_shapes=[
            pltpu.VMEM(tracer.shape, jnp.float32),
            pltpu.SemaphoreType.DMA((5,)),
        ],
        compiler_params=pltpu.CompilerParams(vmem_limit_bytes=40 * 1024 * 1024),
    )(end, lines)


def solution(mesh):
    placed = P(("site", "rows"), "cols", None)
    return jax.shard_map(
        functools.partial(shards, mesh.shape["rows"], mesh.shape["cols"]),
        mesh=mesh,
        in_specs=(placed,) * 3,
        out_specs=(placed, placed),
        check_vma=False,
    )
```

```python
import functools

import jax
import jax.numpy as jnp
from jax import lax
from jax.experimental import pallas as pl
from jax.experimental.pallas import tpu as pltpu
from jax.sharding import PartitionSpec as P

MESH = pl.DeviceIdType.MESH
STEPS, DEPTH = 6, 3
PHASES = STEPS // DEPTH
PAD = 8
HALF = PAD // 2
CUTS = (8,)
FINE = (8,)
HEAD = 2
HOLD = 1600
SIDES = tuple((dy, dx) for dy in (-1, 1, 0) for dx in (-1, 1, 0) if (dy, dx) != (0, 0))
CORNERS = tuple(side for side in SIDES if side[0] and side[1])


def radii(cols):
    out, r = [], 1
    while r < cols - 1:
        out.append(r)
        r *= 2
    return out


def kernel(rows, cols, by, bx, cuts, fine, t_hbm, fy_hbm, fx_hbm, final, moments,
           main, halo, f, fh, weight, early, landed, stats, gathered,
           load_sem, col_send, col_recv, row_send, row_recv, corner_send, corner_recv,
           edge_send, edge_recv,           stat_send, stat_recv, tokens):
    row, col = lax.axis_index("rows"), lax.axis_index("cols")
    top = DEPTH
    tall = by + 2 * top
    chunks = len(cuts) - 1
    plan = [cuts] * (PHASES - 1) + [fine]
    odd = lax.rem(row, 2) == 1

    def exists(dy, dx):
        ok = None
        for step, here, count in ((dy, row, rows), (dx, col, cols)):
            if step:
                inside = (here > 0) if step < 0 else (here < count - 1)
                ok = inside if ok is None else jnp.logical_and(ok, inside)
        return ok

    def at(v, n):
        return jnp.where(odd, top + v, top + by - v - n)

    barrier = pltpu.get_barrier_semaphore()
    for dy, dx in SIDES:
        if dy and dx:
            continue

        @pl.when(exists(dy, dx))
        def _():
            pl.semaphore_signal(barrier, inc=1, device_id={"rows": row + dy, "cols": col + dx},
                                device_id_type=MESH)

    loads = [
        pltpu.make_async_copy(t_hbm, main.at[0, pl.ds(top, by)], load_sem.at[0]),
        pltpu.make_async_copy(fy_hbm, f.at[0, pl.ds(top, by)], load_sem.at[1]),
        pltpu.make_async_copy(fx_hbm, f.at[1, pl.ds(top, by)], load_sem.at[2]),
    ]
    for load in loads:
        load.start()

    for dy in (-1, 1):
        line = top - 1 if dy < 0 else top + by

        @pl.when(jnp.logical_not(exists(dy, 0)))
        def _():
            for s in range(STEPS):
                main[s, line] = jnp.zeros((bx, 128), jnp.float32)
                halo[s, line] = jnp.zeros((PAD, 128), jnp.float32)
    for dx in (-1, 1):
        strip = pl.ds(HALF, HALF) if dx < 0 else pl.ds(0, HALF)

        @pl.when(jnp.logical_not(exists(0, dx)))
        def _():
            for p in range(PHASES):
                halo[p * DEPTH, :, strip] = jnp.zeros((tall, HALF, 128), jnp.float32)

    def one(n, count):
        return (n + count - 1) // count

    def on_both(r):
        return jnp.where(col >= r, 1, 0) + jnp.where(col < cols - r, 1, 0)

    upright = one(row, rows) + one(rows - 1 - row, rows)
    across = on_both(1)

    spread_to = radii(cols)

    def send_token(i):
        if i < len(spread_to):
            r = spread_to[i]
            for sign in (-1, 1):
                @pl.when((col >= r) if sign < 0 else (col < cols - r))
                def _():
                    pl.semaphore_signal(tokens.at[i], inc=1, device_id={"cols": col + sign * r},
                                        device_id_type=MESH)

    def take_token(i):
        if i < len(spread_to):
            pl.semaphore_wait(tokens.at[i], on_both(spread_to[i]))

    def remote(src, dst, send, recv, dy, dx):
        return pltpu.make_async_remote_copy(
            src_ref=src, dst_ref=dst, send_sem=send, recv_sem=recv,
            device_id={"rows": row + dy, "cols": col + dx}, device_id_type=MESH)

    def cols_of(dx, depth):
        if dx > 0:
            return pl.ds(bx - depth, depth), pl.ds(PAD - depth, depth)
        return pl.ds(0, depth), pl.ds(0, depth)

    def rows_of(dy, depth):
        if dy > 0:
            return pl.ds(top + by - depth, depth), pl.ds(top - depth, depth)
        return pl.ds(top, depth), pl.ds(top + by, depth)

    def reach(p, c):
        if c < 0:
            return 0
        return by if c == chunks - 1 else min(by, cuts[c + 1] + STEPS - 1 - p * DEPTH)

    def near_side(first):
        return jnp.where(odd, row > 0, row < rows - 1) if first else jnp.where(odd, row < rows - 1, row > 0)

    def column_copies(p, c):
        v, n = reach(p, c - 1), reach(p, c) - reach(p, c - 1)
        out = []
        if not n:
            return out
        lines = pl.ds(at(v, n), n)
        for i, dx in enumerate((-1, 1)):
            xs, xd = cols_of(dx, DEPTH - 1)
            mine = [remote(main.at[p * DEPTH, lines, xs], halo.at[p * DEPTH, lines, xd],
                           col_send.at[p, c, i, 0], col_recv.at[p, c, i, 0], 0, dx)]
            if p == 0:
                xs, xd = cols_of(dx, 1)
                mine.append(remote(f.at[:, lines, xs], fh.at[:, lines, xd],
                                   col_send.at[p, c, i, 1], col_recv.at[p, c, i, 1], 0, dx))
            out.append((exists(0, dx), exists(0, -dx), mine))
        return out

    def ahead_copies(p, c):
        v, n = reach(p, c - 1), reach(p, c) - reach(p, c - 1)
        if not n:
            return []
        lines = pl.ds(at(v, n), n)
        out = []
        for i, dx in enumerate((-1, 1)):
            x = pl.ds(1, 1) if dx < 0 else pl.ds(PAD - 2, 1)
            out.append((exists(0, dx), exists(0, -dx), [
                remote(early.at[p, i, lines, x], landed.at[p, lines, x],
                       col_send.at[p, c, i, 2], col_recv.at[p, c, i, 2], 0, dx)]))
        return out

    def edge_copies(p, first):
        e, out = 0 if first else 1, []
        y = pl.ds(at(0 if first else by - 1, 1), 1)
        for i, dx in enumerate((-1, 1)):
            xs, xd = (pl.ds(2, 1),) * 2 if dx < 0 else (pl.ds(bx - 3, 1), pl.ds(PAD - 3, 1))
            mine = [remote(main.at[p * DEPTH, y, xs], halo.at[p * DEPTH, y, xd],
                           edge_send.at[p, e, i, 0], edge_recv.at[p, e, i, 0], 0, dx)]
            if p == 0:
                xs, xd = (pl.ds(1, 1),) * 2 if dx < 0 else (pl.ds(bx - 2, 1), pl.ds(PAD - 2, 1))
                mine.append(remote(f.at[:, y, xs], fh.at[:, y, xd],
                                   edge_send.at[p, e, i, 1], edge_recv.at[p, e, i, 1], 0, dx))
            out.append((jnp.logical_and(near_side(first), exists(0, dx)),
                        jnp.logical_and(near_side(first), exists(0, -dx)), mine))
        return out

    def border_copies(p, first, corners):
        out = []
        for i, dy in enumerate((-1, 1)):
            here = odd if (dy < 0) == first else jnp.logical_not(odd)
            there = odd if (dy > 0) == first else jnp.logical_not(odd)
            ys, yd = rows_of(dy, DEPTH)
            mine = [remote(main.at[p * DEPTH, ys], main.at[p * DEPTH, yd],
                           row_send.at[p, i, 0], row_recv.at[p, i, 0], dy, 0)]
            if p == 0:
                ys, yd = rows_of(dy, DEPTH - 1)
                mine.append(remote(f.at[:, ys], f.at[:, yd],
                                   row_send.at[p, i, 1], row_recv.at[p, i, 1], dy, 0))
            if not corners:
                out.append((jnp.logical_and(here, exists(dy, 0)), jnp.logical_and(there, exists(-dy, 0)), mine))
                continue
            for j, dx in enumerate((-1, 1)):
                (ys, yd), (xs, xd) = rows_of(dy, DEPTH - 1), cols_of(dx, DEPTH - 1)
                mine = [remote(main.at[p * DEPTH, ys, xs], halo.at[p * DEPTH, yd, xd],
                               corner_send.at[p, i, j, 0], corner_recv.at[p, i, j, 0], dy, dx)]
                if p == 0 and DEPTH > 2:
                    (ys, yd), (xs, xd) = rows_of(dy, DEPTH - 2), cols_of(dx, DEPTH - 2)
                    mine.append(remote(f.at[:, ys, xs], fh.at[:, yd, xd],
                                       corner_send.at[p, i, j, 1], corner_recv.at[p, i, j, 1], dy, dx))
                out.append((jnp.logical_and(here, exists(dy, dx)),
                            jnp.logical_and(there, exists(-dy, -dx)), mine))
        return out

    def corner_copies(p, c):
        out = []
        if c == 0:
            out = border_copies(p, True, True) + edge_copies(p, True)
        if c == chunks - 1 and rows > 2:
            out = out + border_copies(p, False, True) + edge_copies(p, False)
        return out

    def side_copies(p, c):
        out = column_copies(p, c)
        if c == 0:
            out = out + border_copies(p, True, False)
        if c == chunks - 1 and rows > 2:
            out = out + border_copies(p, False, False)
        return out

    def exchange(p, c):
        return corner_copies(p, c) + side_copies(p, c) + ahead_copies(p, c)

    def start(jobs):
        for here, _, copies in jobs:
            @pl.when(here)
            def _():
                for copy in copies:
                    copy.start()

    def finish(jobs):
        for _, there, copies in jobs:
            @pl.when(there)
            def _():
                for copy in copies:
                    copy.wait_recv()

    def drain(jobs):
        for here, _, copies in jobs:
            @pl.when(here)
            def _():
                for copy in copies:
                    copy.wait_send()

    column = lax.broadcasted_iota(jnp.int32, (1, PAD, 128), 1)
    keep = jnp.logical_and(
        jnp.logical_or(column < HALF, jnp.broadcast_to(col > 0, column.shape)),
        jnp.logical_or(column >= HALF, jnp.broadcast_to(col < cols - 1, column.shape)))

    def mix(c, above, below, right, left, fy, fx):
        spread = (above + below) + (right + left)
        return (0.8 * c + 0.05 * spread) - fy * (above - below) - fx * (right - left)

    def new_main(s, y, k, beyond=False):
        c = main[s, pl.ds(y, k)]
        wide = jnp.concatenate([c, halo[s, pl.ds(y, k)]], axis=1)
        right, left = pltpu.roll(wide, bx + PAD - 1, 1)[:, :bx], pltpu.roll(wide, 1, 1)[:, :bx]
        above, below = main[s, pl.ds(y + 1, k)], main[s, pl.ds(y - 1, k)]
        if beyond:
            return mix(c, above, below, right, left, f[0, pl.ds(y, k)], f[1, pl.ds(y, k)])
        up, down, ahead, back = (weight[i, pl.ds(y - top, k)] for i in range(4))
        return ((0.8 * c + up * above) + down * below) + (ahead * right + back * left)

    def new_halo(s, y, k):
        c = halo[s, pl.ds(y, k)]
        wide = jnp.concatenate([main[s, pl.ds(y, k), pl.ds(bx - PAD, PAD)], c,
                                main[s, pl.ds(y, k), pl.ds(0, PAD)]], axis=1)
        right = pltpu.roll(wide, 3 * PAD - 1, 1)[:, PAD:2 * PAD]
        left = pltpu.roll(wide, 1, 1)[:, PAD:2 * PAD]
        new = mix(c, halo[s, pl.ds(y + 1, k)], halo[s, pl.ds(y - 1, k)], right, left,
                  fh[0, pl.ds(y, k)], fh[1, pl.ds(y, k)])
        return jnp.where(keep, new, 0.0)

    ahead_column = jnp.logical_or(column == 1, column == PAD - 2)

    def take_ahead(p, v, n):
        def do(y, k, always=True):
            got = ahead_column if always is True else jnp.logical_and(ahead_column, always)
            new = jnp.where(got, landed[p, pl.ds(y, k)], new_halo(p * DEPTH, y, k))
            halo[p * DEPTH + 1, pl.ds(y, k)] = jnp.where(keep, new, 0.0)
        end = v + n
        if v == 0:
            v = 1
            do(at(0, 1), 1, jnp.broadcast_to(jnp.logical_not(near_side(True)), column.shape))
        if end == by and rows > 2:
            end = by - 1
            do(at(by - 1, 1), 1, jnp.broadcast_to(jnp.logical_not(near_side(False)), column.shape))
        over(v, end - v, 16, do)

    def send_ahead(p, c):
        v, n = reach(p, c - 1), reach(p, c) - reach(p, c - 1)

        def do(y, k):
            for i, x in enumerate((pl.ds(0, PAD), pl.ds(bx - PAD, PAD))):
                tile = main[p * DEPTH, pl.ds(y, k), x]
                early[p, i, pl.ds(y, k)] = mix(
                    tile, main[p * DEPTH, pl.ds(y + 1, k), x], main[p * DEPTH, pl.ds(y - 1, k), x],
                    pltpu.roll(tile, PAD - 1, 1), pltpu.roll(tile, 1, 1),
                    f[0, pl.ds(y, k), x], f[1, pl.ds(y, k), x])
        end = v + n
        if v == 0:
            v = 1

            @pl.when(jnp.logical_not(near_side(True)))
            def _():
                do(at(0, 1), 1)
        if end == by and rows > 2:
            end = by - 1

            @pl.when(jnp.logical_not(near_side(False)))
            def _():
                do(at(by - 1, 1), 1)
        over(v, end - v, 8, do)

    def over(v, n, k, do):
        if n <= 0:
            return
        y = at(v, n)
        whole = n // k
        if whole > 1:
            @pl.loop(0, whole)
            def _(i):
                do(y + i * k, k)
        elif whole:
            do(y, k)
        if n % k:
            do(y + whole * k, n % k)

    def write_main(s, beyond=False):
        def do(y, k):
            main[s, pl.ds(y, k)] = new_main(s - 1, y, k, beyond)
        return do

    def write_halo(s):
        def do(y, k):
            halo[s, pl.ds(y, k)] = new_halo(s - 1, y, k)
        return do

    def advance(p, c):
        cuts = plan[p]
        chunks = len(cuts) - 1
        for i in range(1, DEPTH + 1):
            s = p * DEPTH + i
            ahead = STEPS - s
            low = 0 if c == 0 else min(by, cuts[c] + ahead)
            high = by if c == chunks - 1 else min(by, cuts[c + 1] + ahead)
            if s == STEPS:
                break
            over(low, high - low, 8, write_main(s))
            if i < DEPTH:
                low = low - 1 if c else 0
                high = high if c == chunks - 1 else high - 1
                if i == 1:
                    take_ahead(p, low, high - low)
                else:
                    over(low, high - low, 16, write_halo(s))
                margin = DEPTH - i
                for first in (True, False):
                    if c != (0 if first else chunks - 1) or not first and rows <= 2:
                        continue
                    for dy in (-1, 1):
                        here = odd if (dy < 0) == first else jnp.logical_not(odd)

                        @pl.when(jnp.logical_and(here, exists(dy, 0)))
                        def _():
                            y = top - margin if dy < 0 else top + by
                            write_main(s, True)(y, margin)
                            write_halo(s)(y, margin)
        return low, high

    pieces = len(fine) - 1

    def share(c, to, sender):
        if c < pieces:
            n = fine[c + 1] - fine[c]
            lines = pl.ds(pl.multiple_of(at(fine[c], n) - top, 8), n)
        else:
            lines = pl.ds(0, by)
        return pltpu.make_async_remote_copy(
            src_ref=stats.at[:, lines], dst_ref=gathered.at[sender, :, lines],
            send_sem=stat_send.at[c, to], recv_sem=stat_recv.at[c, sender],
            device_id={"cols": to}, device_id_type=MESH)

    def each_peer(low, high, do):
        if high - low <= 8:
            for k in range(low, high):
                @pl.when(col != k)
                def _():
                    do(k)
        else:
            @pl.loop(low, high)
            def _(k):
                @pl.when(col != k)
                def _():
                    do(k)

    head = min(HEAD, cols) if pieces > 1 else 0

    def last_step(v, n):
        y = at(v, n)

        @pl.loop(0, n // 8)
        def _(i):
            new = new_main(STEPS - 1, y + i * 8, 8)
            out = pl.ds(pl.multiple_of(y - top + i * 8, 8), 8)
            final[out] = new
            mean = jnp.sum(new, axis=1) / bx
            off = new - mean[:, None, :]
            second = jnp.sum(off * off, axis=1)
            stats[0, out] = mean
            stats[1, out] = second
            gathered[col, 0, out] = mean
            gathered[col, 1, out] = second

    def combine(c):
        n = fine[c + 1] - fine[c]
        y = at(fine[c], n) - top

        @pl.loop(0, n // 8)
        def _(i):
            lines = pl.ds(pl.multiple_of(y + i * 8, 8), 8)
            means = [gathered[k, 0, lines] for k in range(cols)]
            mean = sum(means[1:], means[0]) / cols
            parts = [gathered[k, 1, lines] + bx * ((means[k] - mean) * (means[k] - mean)) for k in range(cols)]
            spread = sum(parts[1:], parts[0])
            moments[0, lines] = mean
            moments[1, lines] = lax.rsqrt(spread / (bx * cols) + 0.0001)

    pl.semaphore_wait(barrier, across + upright)
    send_token(0)
    for load in loads:
        load.wait()
    for c in range(chunks):
        start(side_copies(0, c))
        send_ahead(0, c)
        start(ahead_copies(0, c))
    @pl.loop(0, by // 4)
    def _(i):
        lines = pl.ds(i * 4, 4)
        for d in range(2):
            flow = f[d, pl.ds(top + i * 4, 4)]
            weight[2 * d, lines] = 0.05 - flow
            weight[2 * d + 1, lines] = 0.05 + flow

    known = 0

    def learn():
        take_token(known)
        send_token(known + 1)
        return known + 1

    if spread_to:
        known = learn()
    for c in range(chunks):
        start(corner_copies(0, c))
    while known < len(spread_to) - 1:
        known = learn()
    for p in range(PHASES):
        taken = 0
        for c in range(len(plan[p]) - 1):
            while taken < chunks and cuts[taken] < plan[p][c + 1]:
                finish(exchange(p, taken))
                taken += 1
            low, high = advance(p, c)
            if p + 1 < PHASES:
                start(side_copies(p + 1, c))
                start(corner_copies(p + 1, c))
                send_ahead(p + 1, c)
                start(ahead_copies(p + 1, c))
            else:
                last_step(low, high - low)
                while known < len(spread_to):
                    known = learn()
                if head:
                    each_peer(0, head, lambda k: share(c, k, col).start())
    def later(k):
        @pl.when(k > col)
        def _():
            share(pieces, k, col).start()

    def earlier(k):
        @pl.when(k < col)
        def _():
            share(pieces, k, col).start()
    each_peer(head, cols, later)

    @pl.when(col > head)
    def _():
        pl.delay(HOLD)
    each_peer(head, cols, earlier)
    if head:
        @pl.when(col < head)
        def _():
            for c in range(pieces):
                each_peer(0, cols, lambda k: share(c, k, k).wait_recv())
                combine(c)

        @pl.when(col >= head)
        def _():
            each_peer(0, cols, lambda k: share(pieces, k, k).wait_recv())
            for c in range(pieces):
                combine(c)
    else:
        each_peer(0, cols, lambda k: share(pieces, k, k).wait_recv())
        for c in range(pieces):
            combine(c)
    for c in range(chunks):
        for p in range(PHASES):
            drain(exchange(p, c))
    for c in range(pieces):
        if head:
            each_peer(0, head, lambda k: share(c, k, col).wait_send())
    each_peer(head, cols, lambda k: share(pieces, k, col).wait_send())


def scale_kernel(end, lines, scaled_out, end_out, scaled, sem):
    parts = 4
    g = end.shape[0] // parts
    whole = pltpu.make_async_copy(end, end_out, sem.at[parts])
    stores = [whole]
    for i in range(parts):
        part = pl.ds(i * g, g)
        scaled[part] = (end[part] - lines[0, part][:, None, :]) * lines[1, part][:, None, :]
        store = pltpu.make_async_copy(scaled.at[part], scaled_out.at[part], sem.at[i])
        store.start()
        stores.append(store)
        if i == 0:
            whole.start()
    for store in stores:
        store.wait()


def shards(rows, cols, tracer, flow_y, flow_x):
    by, bx, species = tracer.shape
    cuts, fine = ((0,) + tuple(cut for cut in chosen if cut < by) + (by,) for chosen in (CUTS, FINE))
    chunks = len(cuts) - 1
    pieces = len(fine) - 1
    tall = by + 2 * DEPTH
    block = jax.ShapeDtypeStruct(tracer.shape, jnp.float32)
    hbm = pl.BlockSpec(memory_space=pl.ANY)
    dma = pltpu.SemaphoreType.DMA
    end, lines = pl.pallas_call(
        functools.partial(kernel, rows, cols, by, bx, cuts, fine),
        out_shape=(pltpu.VMEM(tracer.shape, jnp.float32), pltpu.VMEM((2, by, species), jnp.float32)),
        in_specs=[pl.BlockSpec(memory_space=pltpu.HBM)] * 3,
        out_specs=(pl.BlockSpec(memory_space=pltpu.VMEM),) * 2,
        scratch_shapes=[
            pltpu.VMEM((STEPS, tall, bx, species), jnp.float32),
            pltpu.VMEM((STEPS, tall, PAD, species), jnp.float32),
            pltpu.VMEM((2, tall, bx, species), jnp.float32),
            pltpu.VMEM((2, tall, PAD, species), jnp.float32),
            pltpu.VMEM((4, by, bx, species), jnp.float32),
            pltpu.VMEM((PHASES, 2, tall, PAD, species), jnp.float32),
            pltpu.VMEM((PHASES, tall, PAD, species), jnp.float32),
            pltpu.VMEM((2, by, species), jnp.float32),
            pltpu.VMEM((cols, 2, by, species), jnp.float32),
            dma((3,)),
            dma((PHASES, chunks, 2, 3)), dma((PHASES, chunks, 2, 3)),
            dma((PHASES, 2, 2)), dma((PHASES, 2, 2)),
            dma((PHASES, 2, 2, 2)), dma((PHASES, 2, 2, 2)),
            dma((PHASES, 2, 2, 2)), dma((PHASES, 2, 2, 2)),
            dma((pieces + 1, cols)), dma((pieces + 1, cols)),
            pltpu.SemaphoreType.REGULAR((max(1, len(radii(cols))),)),
        ],
        compiler_params=pltpu.CompilerParams(
            collective_id=0, has_side_effects=True, vmem_limit_bytes=67043328 - 1024 * 1024),
    )(tracer, flow_y, flow_x)
    return pl.pallas_call(
        scale_kernel,
        out_shape=(block, block),
        in_specs=[pl.BlockSpec(memory_space=pltpu.VMEM)] * 2,
        out_specs=(hbm, hbm),
        scratch_shapes=[
            pltpu.VMEM(tracer.shape, jnp.float32),
            pltpu.SemaphoreType.DMA((5,)),
        ],
        compiler_params=pltpu.CompilerParams(vmem_limit_bytes=40 * 1024 * 1024),
    )(end, lines)


def solution(mesh):
    placed = P(("site", "rows"), "cols", None)
    return jax.shard_map(
        functools.partial(shards, mesh.shape["rows"], mesh.shape["cols"]),
        mesh=mesh,
        in_specs=(placed,) * 3,
        out_specs=(placed, placed),
        check_vma=False,
    )
```

```python
import functools

import jax
import jax.numpy as jnp
from jax import lax
from jax.experimental import pallas as pl
from jax.experimental.pallas import tpu as pltpu
from jax.sharding import PartitionSpec as P

MESH = pl.DeviceIdType.MESH
STEPS, DEPTH = 6, 3
PHASES = STEPS // DEPTH
PAD = 8
HALF = PAD // 2
CUTS = (16,)
FINE = (16,)
HEAD = 2
HOLD = 2200
SIDES = tuple((dy, dx) for dy in (-1, 1, 0) for dx in (-1, 1, 0) if (dy, dx) != (0, 0))
CORNERS = tuple(side for side in SIDES if side[0] and side[1])


def radii(cols):
    out, r = [], 1
    while r < cols - 1:
        out.append(r)
        r *= 2
    return out


def kernel(rows, cols, by, bx, cuts, fine, t_hbm, fy_hbm, fx_hbm, final, moments,
           main, halo, f, fh, weight, early, landed, stats, gathered,
           load_sem, col_send, col_recv, row_send, row_recv, corner_send, corner_recv,
           edge_send, edge_recv,           stat_send, stat_recv, tokens):
    row, col = lax.axis_index("rows"), lax.axis_index("cols")
    top = DEPTH
    tall = by + 2 * top
    chunks = len(cuts) - 1
    plan = [cuts] * (PHASES - 1) + [fine]
    down = lax.rem(row, 2) == 0

    def exists(dy, dx):
        ok = None
        for step, here, count in ((dy, row, rows), (dx, col, cols)):
            if step:
                inside = (here > 0) if step < 0 else (here < count - 1)
                ok = inside if ok is None else jnp.logical_and(ok, inside)
        return ok

    def at(v, n):
        return jnp.where(down, top + v, top + by - v - n)

    barrier = pltpu.get_barrier_semaphore()
    for dy, dx in SIDES:
        if dy and dx:
            continue

        @pl.when(exists(dy, dx))
        def _():
            pl.semaphore_signal(barrier, inc=1, device_id={"rows": row + dy, "cols": col + dx},
                                device_id_type=MESH)

    loads = [
        pltpu.make_async_copy(t_hbm, main.at[0, pl.ds(top, by)], load_sem.at[0]),
        pltpu.make_async_copy(fy_hbm, f.at[0, pl.ds(top, by)], load_sem.at[1]),
        pltpu.make_async_copy(fx_hbm, f.at[1, pl.ds(top, by)], load_sem.at[2]),
    ]
    for load in loads:
        load.start()

    for dy in (-1, 1):
        line = top - 1 if dy < 0 else top + by

        @pl.when(jnp.logical_not(exists(dy, 0)))
        def _():
            for s in range(STEPS):
                main[s, line] = jnp.zeros((bx, 128), jnp.float32)
                halo[s, line] = jnp.zeros((PAD, 128), jnp.float32)
    for dx in (-1, 1):
        strip = pl.ds(HALF, HALF) if dx < 0 else pl.ds(0, HALF)

        @pl.when(jnp.logical_not(exists(0, dx)))
        def _():
            for p in range(PHASES):
                halo[p * DEPTH, :, strip] = jnp.zeros((tall, HALF, 128), jnp.float32)

    def one(n, count):
        return (n + count - 1) // count

    def on_both(r):
        return jnp.where(col >= r, 1, 0) + jnp.where(col < cols - r, 1, 0)

    upright = one(row, rows) + one(rows - 1 - row, rows)
    across = on_both(1)

    spread_to = radii(cols)

    def send_token(i):
        if i < len(spread_to):
            r = spread_to[i]
            for sign in (-1, 1):
                @pl.when((col >= r) if sign < 0 else (col < cols - r))
                def _():
                    pl.semaphore_signal(tokens.at[i], inc=1, device_id={"cols": col + sign * r},
                                        device_id_type=MESH)

    def take_token(i):
        if i < len(spread_to):
            pl.semaphore_wait(tokens.at[i], on_both(spread_to[i]))

    def remote(src, dst, send, recv, dy, dx):
        return pltpu.make_async_remote_copy(
            src_ref=src, dst_ref=dst, send_sem=send, recv_sem=recv,
            device_id={"rows": row + dy, "cols": col + dx}, device_id_type=MESH)

    def cols_of(dx, depth):
        if dx > 0:
            return pl.ds(bx - depth, depth), pl.ds(PAD - depth, depth)
        return pl.ds(0, depth), pl.ds(0, depth)

    def rows_of(dy, depth):
        if dy > 0:
            return pl.ds(top + by - depth, depth), pl.ds(top - depth, depth)
        return pl.ds(top, depth), pl.ds(top + by, depth)

    def reach(p, c):
        if c < 0:
            return 0
        return by if c == chunks - 1 else min(by, cuts[c + 1] + STEPS - 1 - p * DEPTH)

    def near_side(first):
        return jnp.where(down, row > 0, row < rows - 1) if first else jnp.where(down, row < rows - 1, row > 0)

    def column_copies(p, c):
        v, n = reach(p, c - 1), reach(p, c) - reach(p, c - 1)
        out = []
        if not n:
            return out
        lines = pl.ds(at(v, n), n)
        for i, dx in enumerate((-1, 1)):
            xs, xd = cols_of(dx, DEPTH - 1)
            mine = [remote(main.at[p * DEPTH, lines, xs], halo.at[p * DEPTH, lines, xd],
                           col_send.at[p, c, i, 0], col_recv.at[p, c, i, 0], 0, dx)]
            if p == 0:
                xs, xd = cols_of(dx, 1)
                mine.append(remote(f.at[:, lines, xs], fh.at[:, lines, xd],
                                   col_send.at[p, c, i, 1], col_recv.at[p, c, i, 1], 0, dx))
            out.append((exists(0, dx), exists(0, -dx), mine))
        return out

    def ahead_copies(p, c):
        v, n = reach(p, c - 1), reach(p, c) - reach(p, c - 1)
        if not n:
            return []
        lines = pl.ds(at(v, n), n)
        out = []
        for i, dx in enumerate((-1, 1)):
            x = pl.ds(1, 1) if dx < 0 else pl.ds(PAD - 2, 1)
            out.append((exists(0, dx), exists(0, -dx), [
                remote(early.at[p, i, lines, x], landed.at[p, lines, x],
                       col_send.at[p, c, i, 2], col_recv.at[p, c, i, 2], 0, dx)]))
        return out

    def edge_copies(p, first):
        e, out = 0 if first else 1, []
        y = pl.ds(at(0 if first else by - 1, 1), 1)
        for i, dx in enumerate((-1, 1)):
            xs, xd = (pl.ds(2, 1),) * 2 if dx < 0 else (pl.ds(bx - 3, 1), pl.ds(PAD - 3, 1))
            mine = [remote(main.at[p * DEPTH, y, xs], halo.at[p * DEPTH, y, xd],
                           edge_send.at[p, e, i, 0], edge_recv.at[p, e, i, 0], 0, dx)]
            if p == 0:
                xs, xd = (pl.ds(1, 1),) * 2 if dx < 0 else (pl.ds(bx - 2, 1), pl.ds(PAD - 2, 1))
                mine.append(remote(f.at[:, y, xs], fh.at[:, y, xd],
                                   edge_send.at[p, e, i, 1], edge_recv.at[p, e, i, 1], 0, dx))
            out.append((jnp.logical_and(near_side(first), exists(0, dx)),
                        jnp.logical_and(near_side(first), exists(0, -dx)), mine))
        return out

    def border_copies(p, first, corners):
        out = []
        for i, dy in enumerate((-1, 1)):
            here = down if (dy < 0) == first else jnp.logical_not(down)
            there = down if (dy > 0) == first else jnp.logical_not(down)
            ys, yd = rows_of(dy, DEPTH)
            mine = [remote(main.at[p * DEPTH, ys], main.at[p * DEPTH, yd],
                           row_send.at[p, i, 0], row_recv.at[p, i, 0], dy, 0)]
            if p == 0:
                ys, yd = rows_of(dy, DEPTH - 1)
                mine.append(remote(f.at[:, ys], f.at[:, yd],
                                   row_send.at[p, i, 1], row_recv.at[p, i, 1], dy, 0))
            if not corners:
                out.append((jnp.logical_and(here, exists(dy, 0)), jnp.logical_and(there, exists(-dy, 0)), mine))
                continue
            for j, dx in enumerate((-1, 1)):
                (ys, yd), (xs, xd) = rows_of(dy, DEPTH - 1), cols_of(dx, DEPTH - 1)
                mine = [remote(main.at[p * DEPTH, ys, xs], halo.at[p * DEPTH, yd, xd],
                               corner_send.at[p, i, j, 0], corner_recv.at[p, i, j, 0], dy, dx)]
                if p == 0 and DEPTH > 2:
                    (ys, yd), (xs, xd) = rows_of(dy, DEPTH - 2), cols_of(dx, DEPTH - 2)
                    mine.append(remote(f.at[:, ys, xs], fh.at[:, yd, xd],
                                       corner_send.at[p, i, j, 1], corner_recv.at[p, i, j, 1], dy, dx))
                out.append((jnp.logical_and(here, exists(dy, dx)),
                            jnp.logical_and(there, exists(-dy, -dx)), mine))
        return out

    def corner_copies(p, c):
        out = []
        if c == 0 and rows > 2:
            out = border_copies(p, True, True) + edge_copies(p, True)
        if c == chunks - 1:
            out = out + border_copies(p, False, True) + edge_copies(p, False)
        return out

    def side_copies(p, c):
        out = column_copies(p, c)
        if c == 0 and rows > 2:
            out = out + border_copies(p, True, False)
        if c == chunks - 1:
            out = out + border_copies(p, False, False)
        return out

    def exchange(p, c):
        return corner_copies(p, c) + side_copies(p, c) + ahead_copies(p, c)

    def start(jobs):
        for here, _, copies in jobs:
            @pl.when(here)
            def _():
                for copy in copies:
                    copy.start()

    def finish(jobs):
        for _, there, copies in jobs:
            @pl.when(there)
            def _():
                for copy in copies:
                    copy.wait_recv()

    def drain(jobs):
        for here, _, copies in jobs:
            @pl.when(here)
            def _():
                for copy in copies:
                    copy.wait_send()

    column = lax.broadcasted_iota(jnp.int32, (1, PAD, 128), 1)
    keep = jnp.logical_and(
        jnp.logical_or(column < HALF, jnp.broadcast_to(col > 0, column.shape)),
        jnp.logical_or(column >= HALF, jnp.broadcast_to(col < cols - 1, column.shape)))

    def mix(c, above, below, right, left, fy, fx):
        spread = (above + below) + (right + left)
        return (0.8 * c + 0.05 * spread) - fy * (above - below) - fx * (right - left)

    def new_main(s, y, k, beyond=False):
        c = main[s, pl.ds(y, k)]
        wide = jnp.concatenate([c, halo[s, pl.ds(y, k)]], axis=1)
        right, left = pltpu.roll(wide, bx + PAD - 1, 1)[:, :bx], pltpu.roll(wide, 1, 1)[:, :bx]
        above, below = main[s, pl.ds(y + 1, k)], main[s, pl.ds(y - 1, k)]
        if beyond:
            return mix(c, above, below, right, left, f[0, pl.ds(y, k)], f[1, pl.ds(y, k)])
        up, down, ahead, back = (weight[i, pl.ds(y - top, k)] for i in range(4))
        return ((0.8 * c + up * above) + down * below) + (ahead * right + back * left)

    def new_halo(s, y, k):
        c = halo[s, pl.ds(y, k)]
        wide = jnp.concatenate([main[s, pl.ds(y, k), pl.ds(bx - PAD, PAD)], c,
                                main[s, pl.ds(y, k), pl.ds(0, PAD)]], axis=1)
        right = pltpu.roll(wide, 3 * PAD - 1, 1)[:, PAD:2 * PAD]
        left = pltpu.roll(wide, 1, 1)[:, PAD:2 * PAD]
        new = mix(c, halo[s, pl.ds(y + 1, k)], halo[s, pl.ds(y - 1, k)], right, left,
                  fh[0, pl.ds(y, k)], fh[1, pl.ds(y, k)])
        return jnp.where(keep, new, 0.0)

    ahead_column = jnp.logical_or(column == 1, column == PAD - 2)

    def take_ahead(p, v, n):
        def do(y, k, always=True):
            got = ahead_column if always is True else jnp.logical_and(ahead_column, always)
            new = jnp.where(got, landed[p, pl.ds(y, k)], new_halo(p * DEPTH, y, k))
            halo[p * DEPTH + 1, pl.ds(y, k)] = jnp.where(keep, new, 0.0)
        end = v + n
        if v == 0 and rows > 2:
            v = 1
            do(at(0, 1), 1, jnp.broadcast_to(jnp.logical_not(near_side(True)), column.shape))
        if end == by:
            end = by - 1
            do(at(by - 1, 1), 1, jnp.broadcast_to(jnp.logical_not(near_side(False)), column.shape))
        over(v, end - v, 16, do)

    def send_ahead(p, c):
        v, n = reach(p, c - 1), reach(p, c) - reach(p, c - 1)

        def do(y, k):
            for i, x in enumerate((pl.ds(0, PAD), pl.ds(bx - PAD, PAD))):
                tile = main[p * DEPTH, pl.ds(y, k), x]
                early[p, i, pl.ds(y, k)] = mix(
                    tile, main[p * DEPTH, pl.ds(y + 1, k), x], main[p * DEPTH, pl.ds(y - 1, k), x],
                    pltpu.roll(tile, PAD - 1, 1), pltpu.roll(tile, 1, 1),
                    f[0, pl.ds(y, k), x], f[1, pl.ds(y, k), x])
        end = v + n
        if v == 0 and rows > 2:
            v = 1

            @pl.when(jnp.logical_not(near_side(True)))
            def _():
                do(at(0, 1), 1)
        if end == by:
            end = by - 1

            @pl.when(jnp.logical_not(near_side(False)))
            def _():
                do(at(by - 1, 1), 1)
        over(v, end - v, 8, do)

    def over(v, n, k, do):
        if n <= 0:
            return
        y = at(v, n)
        whole = n // k
        if whole > 1:
            @pl.loop(0, whole)
            def _(i):
                do(y + i * k, k)
        elif whole:
            do(y, k)
        if n % k:
            do(y + whole * k, n % k)

    def write_main(s, beyond=False):
        def do(y, k):
            main[s, pl.ds(y, k)] = new_main(s - 1, y, k, beyond)
        return do

    def write_halo(s):
        def do(y, k):
            halo[s, pl.ds(y, k)] = new_halo(s - 1, y, k)
        return do

    def advance(p, c):
        cuts = plan[p]
        chunks = len(cuts) - 1
        for i in range(1, DEPTH + 1):
            s = p * DEPTH + i
            ahead = STEPS - s
            low = 0 if c == 0 else min(by, cuts[c] + ahead)
            high = by if c == chunks - 1 else min(by, cuts[c + 1] + ahead)
            if s == STEPS:
                break
            over(low, high - low, 8, write_main(s))
            if i < DEPTH:
                low = low - 1 if c else 0
                high = high if c == chunks - 1 else high - 1
                if i == 1:
                    take_ahead(p, low, high - low)
                else:
                    over(low, high - low, 16, write_halo(s))
                margin = DEPTH - i
                for first in (True, False):
                    if c != (0 if first else chunks - 1) or first and rows <= 2:
                        continue
                    for dy in (-1, 1):
                        here = down if (dy < 0) == first else jnp.logical_not(down)

                        @pl.when(jnp.logical_and(here, exists(dy, 0)))
                        def _():
                            y = top - margin if dy < 0 else top + by
                            write_main(s, True)(y, margin)
                            write_halo(s)(y, margin)
        return low, high

    pieces = len(fine) - 1

    def share(c, to, sender):
        if c < pieces:
            n = fine[c + 1] - fine[c]
            lines = pl.ds(pl.multiple_of(at(fine[c], n) - top, 8), n)
        else:
            lines = pl.ds(0, by)
        return pltpu.make_async_remote_copy(
            src_ref=stats.at[:, lines], dst_ref=gathered.at[sender, :, lines],
            send_sem=stat_send.at[c, to], recv_sem=stat_recv.at[c, sender],
            device_id={"cols": to}, device_id_type=MESH)

    def each_peer(low, high, do):
        if high - low <= 8:
            for k in range(low, high):
                @pl.when(col != k)
                def _():
                    do(k)
        else:
            @pl.loop(low, high)
            def _(k):
                @pl.when(col != k)
                def _():
                    do(k)

    head = min(HEAD, cols) if pieces > 1 else 0

    def last_step(v, n):
        y = at(v, n)

        @pl.loop(0, n // 8)
        def _(i):
            new = new_main(STEPS - 1, y + i * 8, 8)
            out = pl.ds(pl.multiple_of(y - top + i * 8, 8), 8)
            final[out] = new
            mean = jnp.sum(new, axis=1) / bx
            off = new - mean[:, None, :]
            second = jnp.sum(off * off, axis=1)
            stats[0, out] = mean
            stats[1, out] = second
            gathered[col, 0, out] = mean
            gathered[col, 1, out] = second

    def combine(c):
        n = fine[c + 1] - fine[c]
        y = at(fine[c], n) - top

        @pl.loop(0, n // 8)
        def _(i):
            lines = pl.ds(pl.multiple_of(y + i * 8, 8), 8)
            means = [gathered[k, 0, lines] for k in range(cols)]
            mean = sum(means[1:], means[0]) / cols
            parts = [gathered[k, 1, lines] + bx * ((means[k] - mean) * (means[k] - mean)) for k in range(cols)]
            spread = sum(parts[1:], parts[0])
            moments[0, lines] = mean
            moments[1, lines] = lax.rsqrt(spread / (bx * cols) + 0.0001)

    pl.semaphore_wait(barrier, across + upright)
    send_token(0)
    for load in loads:
        load.wait()
    for c in range(chunks):
        start(side_copies(0, c))
        send_ahead(0, c)
        start(ahead_copies(0, c))
    @pl.loop(0, by // 4)
    def _(i):
        lines = pl.ds(i * 4, 4)
        for d in range(2):
            flow = f[d, pl.ds(top + i * 4, 4)]
            weight[2 * d, lines] = 0.05 - flow
            weight[2 * d + 1, lines] = 0.05 + flow

    known = 0

    def learn():
        take_token(known)
        send_token(known + 1)
        return known + 1

    if spread_to:
        known = learn()
    for c in range(chunks):
        start(corner_copies(0, c))
    while known < len(spread_to) - 1:
        known = learn()
    for p in range(PHASES):
        taken = 0
        for c in range(len(plan[p]) - 1):
            while taken < chunks and cuts[taken] < plan[p][c + 1]:
                finish(exchange(p, taken))
                taken += 1
            low, high = advance(p, c)
            if p + 1 < PHASES:
                start(side_copies(p + 1, c))
                start(corner_copies(p + 1, c))
                send_ahead(p + 1, c)
                start(ahead_copies(p + 1, c))
            else:
                last_step(low, high - low)
                while known < len(spread_to):
                    known = learn()
                if head:
                    each_peer(0, head, lambda k: share(c, k, col).start())
    def later(k):
        @pl.when(k > col)
        def _():
            share(pieces, k, col).start()

    def earlier(k):
        @pl.when(k < col)
        def _():
            share(pieces, k, col).start()
    each_peer(head, cols, later)

    @pl.when(col > head)
    def _():
        pl.delay(HOLD)
    each_peer(head, cols, earlier)
    if head:
        @pl.when(col < head)
        def _():
            for c in range(pieces):
                each_peer(0, cols, lambda k: share(c, k, k).wait_recv())
                combine(c)

        @pl.when(col >= head)
        def _():
            each_peer(0, cols, lambda k: share(pieces, k, k).wait_recv())
            for c in range(pieces):
                combine(c)
    else:
        each_peer(0, cols, lambda k: share(pieces, k, k).wait_recv())
        for c in range(pieces):
            combine(c)
    for c in range(chunks):
        for p in range(PHASES):
            drain(exchange(p, c))
    for c in range(pieces):
        if head:
            each_peer(0, head, lambda k: share(c, k, col).wait_send())
    each_peer(head, cols, lambda k: share(pieces, k, col).wait_send())


def scale_kernel(end, lines, scaled_out, end_out, scaled, sem):
    parts = 4
    g = end.shape[0] // parts
    whole = pltpu.make_async_copy(end, end_out, sem.at[parts])
    stores = [whole]
    for i in range(parts):
        part = pl.ds(i * g, g)
        scaled[part] = (end[part] - lines[0, part][:, None, :]) * lines[1, part][:, None, :]
        store = pltpu.make_async_copy(scaled.at[part], scaled_out.at[part], sem.at[i])
        store.start()
        stores.append(store)
        if i == 0:
            whole.start()
    for store in stores:
        store.wait()


def shards(rows, cols, tracer, flow_y, flow_x):
    by, bx, species = tracer.shape
    cuts, fine = ((0,) + tuple(cut for cut in chosen if cut < by) + (by,) for chosen in (CUTS, FINE))
    chunks = len(cuts) - 1
    pieces = len(fine) - 1
    tall = by + 2 * DEPTH
    block = jax.ShapeDtypeStruct(tracer.shape, jnp.float32)
    hbm = pl.BlockSpec(memory_space=pl.ANY)
    dma = pltpu.SemaphoreType.DMA
    end, lines = pl.pallas_call(
        functools.partial(kernel, rows, cols, by, bx, cuts, fine),
        out_shape=(pltpu.VMEM(tracer.shape, jnp.float32), pltpu.VMEM((2, by, species), jnp.float32)),
        in_specs=[pl.BlockSpec(memory_space=pltpu.HBM)] * 3,
        out_specs=(pl.BlockSpec(memory_space=pltpu.VMEM),) * 2,
        scratch_shapes=[
            pltpu.VMEM((STEPS, tall, bx, species), jnp.float32),
            pltpu.VMEM((STEPS, tall, PAD, species), jnp.float32),
            pltpu.VMEM((2, tall, bx, species), jnp.float32),
            pltpu.VMEM((2, tall, PAD, species), jnp.float32),
            pltpu.VMEM((4, by, bx, species), jnp.float32),
            pltpu.VMEM((PHASES, 2, tall, PAD, species), jnp.float32),
            pltpu.VMEM((PHASES, tall, PAD, species), jnp.float32),
            pltpu.VMEM((2, by, species), jnp.float32),
            pltpu.VMEM((cols, 2, by, species), jnp.float32),
            dma((3,)),
            dma((PHASES, chunks, 2, 3)), dma((PHASES, chunks, 2, 3)),
            dma((PHASES, 2, 2)), dma((PHASES, 2, 2)),
            dma((PHASES, 2, 2, 2)), dma((PHASES, 2, 2, 2)),
            dma((PHASES, 2, 2, 2)), dma((PHASES, 2, 2, 2)),
            dma((pieces + 1, cols)), dma((pieces + 1, cols)),
            pltpu.SemaphoreType.REGULAR((max(1, len(radii(cols))),)),
        ],
        compiler_params=pltpu.CompilerParams(
            collective_id=0, has_side_effects=True, vmem_limit_bytes=67043328 - 1024 * 1024),
    )(tracer, flow_y, flow_x)
    return pl.pallas_call(
        scale_kernel,
        out_shape=(block, block),
        in_specs=[pl.BlockSpec(memory_space=pltpu.VMEM)] * 2,
        out_specs=(hbm, hbm),
        scratch_shapes=[
            pltpu.VMEM(tracer.shape, jnp.float32),
            pltpu.SemaphoreType.DMA((5,)),
        ],
        compiler_params=pltpu.CompilerParams(vmem_limit_bytes=40 * 1024 * 1024),
    )(end, lines)


def solution(mesh):
    placed = P(("site", "rows"), "cols", None)
    return jax.shard_map(
        functools.partial(shards, mesh.shape["rows"], mesh.shape["cols"]),
        mesh=mesh,
        in_specs=(placed,) * 3,
        out_specs=(placed, placed),
        check_vma=False,
    )
```

```python
import functools

import jax
import jax.numpy as jnp
from jax import lax
from jax.experimental import pallas as pl
from jax.experimental.pallas import tpu as pltpu
from jax.sharding import PartitionSpec as P

MESH = pl.DeviceIdType.MESH
STEPS, DEPTH = 6, 3
PHASES = STEPS // DEPTH
PAD = 8
HALF = PAD // 2
CUTS = (16,)
FINE = (16,)
HEAD = 2
HOLD = (1500, 2500)
SIDES = tuple((dy, dx) for dy in (-1, 1, 0) for dx in (-1, 1, 0) if (dy, dx) != (0, 0))
CORNERS = tuple(side for side in SIDES if side[0] and side[1])


def radii(cols):
    out, r = [], 1
    while r < cols - 1:
        out.append(r)
        r *= 2
    return out


def kernel(rows, cols, by, bx, cuts, fine, t_hbm, fy_hbm, fx_hbm, final, moments,
           main, halo, f, fh, weight, early, landed, stats, gathered,
           load_sem, col_send, col_recv, row_send, row_recv, corner_send, corner_recv,
           edge_send, edge_recv,           stat_send, stat_recv, tokens, heard):
    row, col = lax.axis_index("rows"), lax.axis_index("cols")
    top = DEPTH
    tall = by + 2 * top
    chunks = len(cuts) - 1
    plan = [cuts] * (PHASES - 1) + [fine]
    down = lax.rem(row, 2) == 0

    def exists(dy, dx):
        ok = None
        for step, here, count in ((dy, row, rows), (dx, col, cols)):
            if step:
                inside = (here > 0) if step < 0 else (here < count - 1)
                ok = inside if ok is None else jnp.logical_and(ok, inside)
        return ok

    def at(v, n):
        return jnp.where(down, top + v, top + by - v - n)

    barrier = pltpu.get_barrier_semaphore()
    for dy, dx in SIDES:
        if dy and dx:
            continue

        @pl.when(exists(dy, dx))
        def _():
            pl.semaphore_signal(barrier, inc=1, device_id={"rows": row + dy, "cols": col + dx},
                                device_id_type=MESH)

    loads = [
        pltpu.make_async_copy(t_hbm, main.at[0, pl.ds(top, by)], load_sem.at[0]),
        pltpu.make_async_copy(fy_hbm, f.at[0, pl.ds(top, by)], load_sem.at[1]),
        pltpu.make_async_copy(fx_hbm, f.at[1, pl.ds(top, by)], load_sem.at[2]),
    ]
    for load in loads:
        load.start()

    for dy in (-1, 1):
        line = top - 1 if dy < 0 else top + by

        @pl.when(jnp.logical_not(exists(dy, 0)))
        def _():
            for s in range(STEPS):
                main[s, line] = jnp.zeros((bx, 128), jnp.float32)
                halo[s, line] = jnp.zeros((PAD, 128), jnp.float32)
    for dx in (-1, 1):
        strip = pl.ds(HALF, HALF) if dx < 0 else pl.ds(0, HALF)

        @pl.when(jnp.logical_not(exists(0, dx)))
        def _():
            for p in range(PHASES):
                halo[p * DEPTH, :, strip] = jnp.zeros((tall, HALF, 128), jnp.float32)

    def one(n, count):
        return (n + count - 1) // count

    def on_both(r):
        return jnp.where(col >= r, 1, 0) + jnp.where(col < cols - r, 1, 0)

    upright = one(row, rows) + one(rows - 1 - row, rows)
    across = on_both(1)

    spread_to = radii(cols)

    def send_token(i):
        if i < len(spread_to):
            r = spread_to[i]
            for sign in (-1, 1):
                @pl.when((col >= r) if sign < 0 else (col < cols - r))
                def _():
                    pl.semaphore_signal(tokens.at[i], inc=1, device_id={"cols": col + sign * r},
                                        device_id_type=MESH)

    def take_token(i):
        if i < len(spread_to):
            pl.semaphore_wait(tokens.at[i], on_both(spread_to[i]))

    def remote(src, dst, send, recv, dy, dx):
        return pltpu.make_async_remote_copy(
            src_ref=src, dst_ref=dst, send_sem=send, recv_sem=recv,
            device_id={"rows": row + dy, "cols": col + dx}, device_id_type=MESH)

    def cols_of(dx, depth):
        if dx > 0:
            return pl.ds(bx - depth, depth), pl.ds(PAD - depth, depth)
        return pl.ds(0, depth), pl.ds(0, depth)

    def rows_of(dy, depth):
        if dy > 0:
            return pl.ds(top + by - depth, depth), pl.ds(top - depth, depth)
        return pl.ds(top, depth), pl.ds(top + by, depth)

    def reach(p, c):
        if c < 0:
            return 0
        return by if c == chunks - 1 else min(by, cuts[c + 1] + STEPS - 1 - p * DEPTH)

    def near_side(first):
        return jnp.where(down, row > 0, row < rows - 1) if first else jnp.where(down, row < rows - 1, row > 0)

    def column_copies(p, c):
        v, n = reach(p, c - 1), reach(p, c) - reach(p, c - 1)
        out = []
        if not n:
            return out
        lines = pl.ds(at(v, n), n)
        for i, dx in enumerate((-1, 1)):
            xs, xd = cols_of(dx, DEPTH - 1)
            mine = [remote(main.at[p * DEPTH, lines, xs], halo.at[p * DEPTH, lines, xd],
                           col_send.at[p, c, i, 0], col_recv.at[p, c, i, 0], 0, dx)]
            if p == 0:
                xs, xd = cols_of(dx, 1)
                mine.append(remote(f.at[:, lines, xs], fh.at[:, lines, xd],
                                   col_send.at[p, c, i, 1], col_recv.at[p, c, i, 1], 0, dx))
            out.append((exists(0, dx), exists(0, -dx), mine))
        return out

    def ahead_copies(p, c):
        v, n = reach(p, c - 1), reach(p, c) - reach(p, c - 1)
        if not n:
            return []
        lines = pl.ds(at(v, n), n)
        out = []
        for i, dx in enumerate((-1, 1)):
            x = pl.ds(1, 1) if dx < 0 else pl.ds(PAD - 2, 1)
            out.append((exists(0, dx), exists(0, -dx), [
                remote(early.at[p, i, lines, x], landed.at[p, lines, x],
                       col_send.at[p, c, i, 2], col_recv.at[p, c, i, 2], 0, dx)]))
        return out

    def edge_copies(p, first):
        e, out = 0 if first else 1, []
        y = pl.ds(at(0 if first else by - 1, 1), 1)
        for i, dx in enumerate((-1, 1)):
            xs, xd = (pl.ds(2, 1),) * 2 if dx < 0 else (pl.ds(bx - 3, 1), pl.ds(PAD - 3, 1))
            mine = [remote(main.at[p * DEPTH, y, xs], halo.at[p * DEPTH, y, xd],
                           edge_send.at[p, e, i, 0], edge_recv.at[p, e, i, 0], 0, dx)]
            if p == 0:
                xs, xd = (pl.ds(1, 1),) * 2 if dx < 0 else (pl.ds(bx - 2, 1), pl.ds(PAD - 2, 1))
                mine.append(remote(f.at[:, y, xs], fh.at[:, y, xd],
                                   edge_send.at[p, e, i, 1], edge_recv.at[p, e, i, 1], 0, dx))
            out.append((jnp.logical_and(near_side(first), exists(0, dx)),
                        jnp.logical_and(near_side(first), exists(0, -dx)), mine))
        return out

    def border_copies(p, first, corners):
        out = []
        for i, dy in enumerate((-1, 1)):
            here = down if (dy < 0) == first else jnp.logical_not(down)
            there = down if (dy > 0) == first else jnp.logical_not(down)
            ys, yd = rows_of(dy, DEPTH)
            mine = [remote(main.at[p * DEPTH, ys], main.at[p * DEPTH, yd],
                           row_send.at[p, i, 0], row_recv.at[p, i, 0], dy, 0)]
            if p == 0:
                ys, yd = rows_of(dy, DEPTH - 1)
                mine.append(remote(f.at[:, ys], f.at[:, yd],
                                   row_send.at[p, i, 1], row_recv.at[p, i, 1], dy, 0))
            if not corners:
                out.append((jnp.logical_and(here, exists(dy, 0)), jnp.logical_and(there, exists(-dy, 0)), mine))
                continue
            for j, dx in enumerate((-1, 1)):
                (ys, yd), (xs, xd) = rows_of(dy, DEPTH - 1), cols_of(dx, DEPTH - 1)
                mine = [remote(main.at[p * DEPTH, ys, xs], halo.at[p * DEPTH, yd, xd],
                               corner_send.at[p, i, j, 0], corner_recv.at[p, i, j, 0], dy, dx)]
                if p == 0 and DEPTH > 2:
                    (ys, yd), (xs, xd) = rows_of(dy, DEPTH - 2), cols_of(dx, DEPTH - 2)
                    mine.append(remote(f.at[:, ys, xs], fh.at[:, yd, xd],
                                       corner_send.at[p, i, j, 1], corner_recv.at[p, i, j, 1], dy, dx))
                out.append((jnp.logical_and(here, exists(dy, dx)),
                            jnp.logical_and(there, exists(-dy, -dx)), mine))
        return out

    def corner_copies(p, c):
        out = []
        if c == 0 and rows > 2:
            out = border_copies(p, True, True) + edge_copies(p, True)
        if c == chunks - 1:
            out = out + border_copies(p, False, True) + edge_copies(p, False)
        return out

    def side_copies(p, c):
        out = column_copies(p, c)
        if c == 0 and rows > 2:
            out = out + border_copies(p, True, False)
        if c == chunks - 1:
            out = out + border_copies(p, False, False)
        return out

    def exchange(p, c):
        return corner_copies(p, c) + side_copies(p, c) + ahead_copies(p, c)

    def start(jobs):
        for here, _, copies in jobs:
            @pl.when(here)
            def _():
                for copy in copies:
                    copy.start()

    def finish(jobs):
        for _, there, copies in jobs:
            @pl.when(there)
            def _():
                for copy in copies:
                    copy.wait_recv()

    def drain(jobs):
        for here, _, copies in jobs:
            @pl.when(here)
            def _():
                for copy in copies:
                    copy.wait_send()

    column = lax.broadcasted_iota(jnp.int32, (1, PAD, 128), 1)
    keep = jnp.logical_and(
        jnp.logical_or(column < HALF, jnp.broadcast_to(col > 0, column.shape)),
        jnp.logical_or(column >= HALF, jnp.broadcast_to(col < cols - 1, column.shape)))

    def mix(c, above, below, right, left, fy, fx):
        spread = (above + below) + (right + left)
        return (0.8 * c + 0.05 * spread) - fy * (above - below) - fx * (right - left)

    def new_main(s, y, k, beyond=False):
        c = main[s, pl.ds(y, k)]
        wide = jnp.concatenate([c, halo[s, pl.ds(y, k)]], axis=1)
        right, left = pltpu.roll(wide, bx + PAD - 1, 1)[:, :bx], pltpu.roll(wide, 1, 1)[:, :bx]
        above, below = main[s, pl.ds(y + 1, k)], main[s, pl.ds(y - 1, k)]
        if beyond:
            return mix(c, above, below, right, left, f[0, pl.ds(y, k)], f[1, pl.ds(y, k)])
        up, down, ahead, back = (weight[i, pl.ds(y - top, k)] for i in range(4))
        return ((0.8 * c + up * above) + down * below) + (ahead * right + back * left)

    def new_halo(s, y, k):
        c = halo[s, pl.ds(y, k)]
        wide = jnp.concatenate([main[s, pl.ds(y, k), pl.ds(bx - PAD, PAD)], c,
                                main[s, pl.ds(y, k), pl.ds(0, PAD)]], axis=1)
        right = pltpu.roll(wide, 3 * PAD - 1, 1)[:, PAD:2 * PAD]
        left = pltpu.roll(wide, 1, 1)[:, PAD:2 * PAD]
        new = mix(c, halo[s, pl.ds(y + 1, k)], halo[s, pl.ds(y - 1, k)], right, left,
                  fh[0, pl.ds(y, k)], fh[1, pl.ds(y, k)])
        return jnp.where(keep, new, 0.0)

    ahead_column = jnp.logical_or(column == 1, column == PAD - 2)

    def take_ahead(p, v, n):
        def do(y, k, always=True):
            got = ahead_column if always is True else jnp.logical_and(ahead_column, always)
            new = jnp.where(got, landed[p, pl.ds(y, k)], new_halo(p * DEPTH, y, k))
            halo[p * DEPTH + 1, pl.ds(y, k)] = jnp.where(keep, new, 0.0)
        end = v + n
        if v == 0 and rows > 2:
            v = 1
            do(at(0, 1), 1, jnp.broadcast_to(jnp.logical_not(near_side(True)), column.shape))
        if end == by:
            end = by - 1
            do(at(by - 1, 1), 1, jnp.broadcast_to(jnp.logical_not(near_side(False)), column.shape))
        over(v, end - v, 16, do)

    def send_ahead(p, c):
        v, n = reach(p, c - 1), reach(p, c) - reach(p, c - 1)

        def do(y, k):
            for i, x in enumerate((pl.ds(0, PAD), pl.ds(bx - PAD, PAD))):
                tile = main[p * DEPTH, pl.ds(y, k), x]
                early[p, i, pl.ds(y, k)] = mix(
                    tile, main[p * DEPTH, pl.ds(y + 1, k), x], main[p * DEPTH, pl.ds(y - 1, k), x],
                    pltpu.roll(tile, PAD - 1, 1), pltpu.roll(tile, 1, 1),
                    f[0, pl.ds(y, k), x], f[1, pl.ds(y, k), x])
        end = v + n
        if v == 0 and rows > 2:
            v = 1

            @pl.when(jnp.logical_not(near_side(True)))
            def _():
                do(at(0, 1), 1)
        if end == by:
            end = by - 1

            @pl.when(jnp.logical_not(near_side(False)))
            def _():
                do(at(by - 1, 1), 1)
        over(v, end - v, 8, do)

    def over(v, n, k, do):
        if n <= 0:
            return
        y = at(v, n)
        whole = n // k
        if whole > 1:
            @pl.loop(0, whole)
            def _(i):
                do(y + i * k, k)
        elif whole:
            do(y, k)
        if n % k:
            do(y + whole * k, n % k)

    def write_main(s, beyond=False):
        def do(y, k):
            main[s, pl.ds(y, k)] = new_main(s - 1, y, k, beyond)
        return do

    def write_edges(s):
        def do(y, k):
            lines = pl.ds(y, k)
            for x, wide in (
                (0, (halo[s - 1, lines], main[s - 1, lines, pl.ds(0, 2 * PAD)])),
                (bx - PAD, (main[s - 1, lines, pl.ds(bx - 2 * PAD, 2 * PAD)], halo[s - 1, lines])),
            ):
                tile = pl.ds(x, PAD)
                wide = jnp.concatenate(wide, axis=1)
                right = pltpu.roll(wide, 3 * PAD - 1, 1)[:, PAD:2 * PAD]
                left = pltpu.roll(wide, 1, 1)[:, PAD:2 * PAD]
                up, down, front, back = (weight[i, pl.ds(y - top, k), tile] for i in range(4))
                main[s, lines, tile] = (
                    (0.8 * wide[:, PAD:2 * PAD] + up * main[s - 1, pl.ds(y + 1, k), tile])
                    + down * main[s - 1, pl.ds(y - 1, k), tile]
                ) + (front * right + back * left)
        return do

    def settle(p):
        def step(s):
            def do(y, k):
                c = main[s - 1, pl.ds(y, k)]
                up, down, front, back = (weight[i, pl.ds(y - top, k)] for i in range(4))
                main[s, pl.ds(y, k)] = (
                    (0.8 * c + up * main[s - 1, pl.ds(y + 1, k)]) + down * main[s - 1, pl.ds(y - 1, k)]
                ) + (front * pltpu.roll(c, bx - 1, 1) + back * pltpu.roll(c, 1, 1))
            return do
        for i in range(1, DEPTH + 1):
            s = p * DEPTH + i
            if s < STEPS:
                low = i if rows > 2 else 0
                over(low, by - i - low, 8, step(s))

    def write_halo(s):
        def do(y, k):
            halo[s, pl.ds(y, k)] = new_halo(s - 1, y, k)
        return do

    def advance(p, c):
        cuts = plan[p]
        chunks = len(cuts) - 1
        for i in range(1, DEPTH + 1):
            s = p * DEPTH + i
            ahead = STEPS - s
            low = 0 if c == 0 else min(by, cuts[c] + ahead)
            high = by if c == chunks - 1 else min(by, cuts[c + 1] + ahead)
            if s == STEPS:
                break
            start_v = max(low, DEPTH if rows > 2 else 0)
            end_v = min(high, by - DEPTH)
            over(low, start_v - low, 8, write_main(s))
            over(start_v, end_v - start_v, 8, write_edges(s))
            over(end_v, high - end_v, 8, write_main(s))
            if i < DEPTH:
                low = low - 1 if c else 0
                high = high if c == chunks - 1 else high - 1
                if i == 1:
                    take_ahead(p, low, high - low)
                else:
                    over(low, high - low, 16, write_halo(s))
                margin = DEPTH - i
                for first in (True, False):
                    if c != (0 if first else chunks - 1) or first and rows <= 2:
                        continue
                    for dy in (-1, 1):
                        here = down if (dy < 0) == first else jnp.logical_not(down)

                        @pl.when(jnp.logical_and(here, exists(dy, 0)))
                        def _():
                            y = top - margin if dy < 0 else top + by
                            write_main(s, True)(y, margin)
                            write_halo(s)(y, margin)
        return low, high

    pieces = len(fine) - 1

    def share(c, to, sender):
        if c < pieces:
            n = fine[c + 1] - fine[c]
            lines = pl.ds(pl.multiple_of(at(fine[c], n) - top, 8), n)
        else:
            lines = pl.ds(0, by)
        return pltpu.make_async_remote_copy(
            src_ref=stats.at[:, lines], dst_ref=gathered.at[sender, :, lines],
            send_sem=stat_send.at[c, to], recv_sem=stat_recv.at[c, sender],
            device_id={"cols": to}, device_id_type=MESH)

    def each_peer(low, high, do):
        if high - low <= 8:
            for k in range(low, high):
                @pl.when(col != k)
                def _():
                    do(k)
        else:
            @pl.loop(low, high)
            def _(k):
                @pl.when(col != k)
                def _():
                    do(k)

    head = min(HEAD, cols) if pieces > 1 else 0

    def last_step(v, n):
        y = at(v, n)

        @pl.loop(0, n // 8)
        def _(i):
            new = new_main(STEPS - 1, y + i * 8, 8)
            out = pl.ds(pl.multiple_of(y - top + i * 8, 8), 8)
            final[out] = new
            mean = jnp.sum(new, axis=1) / bx
            off = new - mean[:, None, :]
            second = jnp.sum(off * off, axis=1)
            stats[0, out] = mean
            stats[1, out] = second
            gathered[col, 0, out] = mean
            gathered[col, 1, out] = second

    def combine(c):
        n = fine[c + 1] - fine[c]
        y = at(fine[c], n) - top

        @pl.loop(0, n // 8)
        def _(i):
            lines = pl.ds(pl.multiple_of(y + i * 8, 8), 8)
            means = [gathered[k, 0, lines] for k in range(cols)]
            mean = sum(means[1:], means[0]) / cols
            parts = [gathered[k, 1, lines] + bx * ((means[k] - mean) * (means[k] - mean)) for k in range(cols)]
            spread = sum(parts[1:], parts[0])
            moments[0, lines] = mean
            moments[1, lines] = lax.rsqrt(spread / (bx * cols) + 0.0001)

    pl.semaphore_wait(barrier, across + upright)
    for dy in (-1, 1):
        @pl.when(exists(dy, 0))
        def _():
            pl.semaphore_signal(heard, inc=1, device_id={"rows": row + dy}, device_id_type=MESH)
    send_token(0)
    for load in loads:
        load.wait()
    for c in range(chunks):
        start(side_copies(0, c))
        send_ahead(0, c)
        start(ahead_copies(0, c))
    @pl.loop(0, by // 4)
    def _(i):
        lines = pl.ds(i * 4, 4)
        for d in range(2):
            flow = f[d, pl.ds(top + i * 4, 4)]
            weight[2 * d, lines] = 0.05 - flow
            weight[2 * d + 1, lines] = 0.05 + flow

    known = 0

    def learn():
        take_token(known)
        send_token(known + 1)
        return known + 1

    pl.semaphore_wait(heard, upright)
    for c in range(chunks):
        start(corner_copies(0, c))
    while known < len(spread_to) - 1:
        known = learn()
    for p in range(PHASES):
        taken = 0
        settle(p)
        for c in range(len(plan[p]) - 1):
            while taken < chunks and cuts[taken] < plan[p][c + 1]:
                finish(exchange(p, taken))
                taken += 1
            low, high = advance(p, c)
            if p + 1 < PHASES:
                start(corner_copies(p + 1, c))
                start(side_copies(p + 1, c))
                send_ahead(p + 1, c)
                start(ahead_copies(p + 1, c))
            else:
                last_step(low, high - low)
                while known < len(spread_to):
                    known = learn()
                if head:
                    each_peer(0, head, lambda k: share(c, k, col).start())
    def later(k):
        @pl.when(k > col)
        def _():
            share(pieces, k, col).start()

    def earlier(k):
        @pl.when(k < col)
        def _():
            share(pieces, k, col).start()
    each_peer(head, cols, later)

    @pl.when(jnp.logical_and(col > head, col < cols - 2))
    def _():
        pl.delay(HOLD[0])

    @pl.when(jnp.logical_and(col > head, col >= cols - 2))
    def _():
        pl.delay(HOLD[1])
    each_peer(head, cols, earlier)
    if head:
        @pl.when(col < head)
        def _():
            for c in range(pieces):
                each_peer(0, cols, lambda k: share(c, k, k).wait_recv())
                combine(c)

        @pl.when(col >= head)
        def _():
            each_peer(0, cols, lambda k: share(pieces, k, k).wait_recv())
            for c in range(pieces):
                combine(c)
    else:
        each_peer(0, cols, lambda k: share(pieces, k, k).wait_recv())
        for c in range(pieces):
            combine(c)
    for c in range(chunks):
        for p in range(PHASES):
            drain(exchange(p, c))
    for c in range(pieces):
        if head:
            each_peer(0, head, lambda k: share(c, k, col).wait_send())
    each_peer(head, cols, lambda k: share(pieces, k, col).wait_send())


def scale_kernel(end, lines, scaled_out, end_out, scaled, sem):
    parts = 4
    g = end.shape[0] // parts
    whole = pltpu.make_async_copy(end, end_out, sem.at[parts])
    stores = [whole]
    for i in range(parts):
        part = pl.ds(i * g, g)
        scaled[part] = (end[part] - lines[0, part][:, None, :]) * lines[1, part][:, None, :]
        store = pltpu.make_async_copy(scaled.at[part], scaled_out.at[part], sem.at[i])
        store.start()
        stores.append(store)
        if i == 0:
            whole.start()
    for store in stores:
        store.wait()


def shards(rows, cols, tracer, flow_y, flow_x):
    by, bx, species = tracer.shape
    cuts, fine = ((0,) + tuple(cut for cut in chosen if cut < by) + (by,) for chosen in (CUTS, FINE))
    chunks = len(cuts) - 1
    pieces = len(fine) - 1
    tall = by + 2 * DEPTH
    block = jax.ShapeDtypeStruct(tracer.shape, jnp.float32)
    hbm = pl.BlockSpec(memory_space=pl.ANY)
    dma = pltpu.SemaphoreType.DMA
    end, lines = pl.pallas_call(
        functools.partial(kernel, rows, cols, by, bx, cuts, fine),
        out_shape=(pltpu.VMEM(tracer.shape, jnp.float32), pltpu.VMEM((2, by, species), jnp.float32)),
        in_specs=[pl.BlockSpec(memory_space=pltpu.HBM)] * 3,
        out_specs=(pl.BlockSpec(memory_space=pltpu.VMEM),) * 2,
        scratch_shapes=[
            pltpu.VMEM((STEPS, tall, bx, species), jnp.float32),
            pltpu.VMEM((STEPS, tall, PAD, species), jnp.float32),
            pltpu.VMEM((2, tall, bx, species), jnp.float32),
            pltpu.VMEM((2, tall, PAD, species), jnp.float32),
            pltpu.VMEM((4, by, bx, species), jnp.float32),
            pltpu.VMEM((PHASES, 2, tall, PAD, species), jnp.float32),
            pltpu.VMEM((PHASES, tall, PAD, species), jnp.float32),
            pltpu.VMEM((2, by, species), jnp.float32),
            pltpu.VMEM((cols, 2, by, species), jnp.float32),
            dma((3,)),
            dma((PHASES, chunks, 2, 3)), dma((PHASES, chunks, 2, 3)),
            dma((PHASES, 2, 2)), dma((PHASES, 2, 2)),
            dma((PHASES, 2, 2, 2)), dma((PHASES, 2, 2, 2)),
            dma((PHASES, 2, 2, 2)), dma((PHASES, 2, 2, 2)),
            dma((pieces + 1, cols)), dma((pieces + 1, cols)),
            pltpu.SemaphoreType.REGULAR((max(1, len(radii(cols))),)),
            pltpu.SemaphoreType.REGULAR,
        ],
        compiler_params=pltpu.CompilerParams(
            collective_id=0, has_side_effects=True, vmem_limit_bytes=67043328 - 1024 * 1024),
    )(tracer, flow_y, flow_x)
    return pl.pallas_call(
        scale_kernel,
        out_shape=(block, block),
        in_specs=[pl.BlockSpec(memory_space=pltpu.VMEM)] * 2,
        out_specs=(hbm, hbm),
        scratch_shapes=[
            pltpu.VMEM(tracer.shape, jnp.float32),
            pltpu.SemaphoreType.DMA((5,)),
        ],
        compiler_params=pltpu.CompilerParams(vmem_limit_bytes=40 * 1024 * 1024),
    )(end, lines)


def solution(mesh):
    placed = P(("site", "rows"), "cols", None)
    return jax.shard_map(
        functools.partial(shards, mesh.shape["rows"], mesh.shape["cols"]),
        mesh=mesh,
        in_specs=(placed,) * 3,
        out_specs=(placed, placed),
        check_vma=False,
    )
```

```python
import functools

import jax
import jax.numpy as jnp
from jax import lax
from jax.experimental import pallas as pl
from jax.experimental.pallas import tpu as pltpu
from jax.sharding import PartitionSpec as P

MESH = pl.DeviceIdType.MESH
STEPS, DEPTH = 6, 3
PHASES = STEPS // DEPTH
PAD = 8
HALF = PAD // 2
CUTS = (16,)
FINE = (16, 24)
HEAD = 2
HOLD = (1500, 2500)
SIDES = tuple((dy, dx) for dy in (-1, 1, 0) for dx in (-1, 1, 0) if (dy, dx) != (0, 0))
CORNERS = tuple(side for side in SIDES if side[0] and side[1])


def radii(cols):
    out, r = [], 1
    while r < cols - 1:
        out.append(r)
        r *= 2
    return out


def kernel(rows, cols, by, bx, cuts, fine, t_hbm, fy_hbm, fx_hbm, final, moments,
           main, halo, f, fh, weight, early, landed, stats, gathered,
           load_sem, col_send, col_recv, row_send, row_recv, corner_send, corner_recv,
           edge_send, edge_recv,           stat_send, stat_recv, tokens, heard):
    row, col = lax.axis_index("rows"), lax.axis_index("cols")
    top = DEPTH
    tall = by + 2 * top
    chunks = len(cuts) - 1
    plan = [cuts] * (PHASES - 1) + [fine]
    down = lax.rem(row, 2) == 0

    def exists(dy, dx):
        ok = None
        for step, here, count in ((dy, row, rows), (dx, col, cols)):
            if step:
                inside = (here > 0) if step < 0 else (here < count - 1)
                ok = inside if ok is None else jnp.logical_and(ok, inside)
        return ok

    def at(v, n):
        return jnp.where(down, top + v, top + by - v - n)

    barrier = pltpu.get_barrier_semaphore()
    for dy, dx in SIDES:
        if dy and dx:
            continue

        @pl.when(exists(dy, dx))
        def _():
            pl.semaphore_signal(barrier, inc=1, device_id={"rows": row + dy, "cols": col + dx},
                                device_id_type=MESH)

    loads = [
        pltpu.make_async_copy(t_hbm, main.at[0, pl.ds(top, by)], load_sem.at[0]),
        pltpu.make_async_copy(fy_hbm, f.at[0, pl.ds(top, by)], load_sem.at[1]),
        pltpu.make_async_copy(fx_hbm, f.at[1, pl.ds(top, by)], load_sem.at[2]),
    ]
    for load in loads:
        load.start()

    for dy in (-1, 1):
        line = top - 1 if dy < 0 else top + by

        @pl.when(jnp.logical_not(exists(dy, 0)))
        def _():
            for s in range(STEPS):
                main[s, line] = jnp.zeros((bx, 128), jnp.float32)
                halo[s, line] = jnp.zeros((PAD, 128), jnp.float32)
    for dx in (-1, 1):
        strip = pl.ds(HALF, HALF) if dx < 0 else pl.ds(0, HALF)

        @pl.when(jnp.logical_not(exists(0, dx)))
        def _():
            for p in range(PHASES):
                halo[p * DEPTH, :, strip] = jnp.zeros((tall, HALF, 128), jnp.float32)

    def one(n, count):
        return (n + count - 1) // count

    def on_both(r):
        return jnp.where(col >= r, 1, 0) + jnp.where(col < cols - r, 1, 0)

    upright = one(row, rows) + one(rows - 1 - row, rows)
    across = on_both(1)

    spread_to = radii(cols)

    def send_token(i):
        if i < len(spread_to):
            r = spread_to[i]
            for sign in (-1, 1):
                @pl.when((col >= r) if sign < 0 else (col < cols - r))
                def _():
                    pl.semaphore_signal(tokens.at[i], inc=1, device_id={"cols": col + sign * r},
                                        device_id_type=MESH)

    def take_token(i):
        if i < len(spread_to):
            pl.semaphore_wait(tokens.at[i], on_both(spread_to[i]))

    def remote(src, dst, send, recv, dy, dx):
        return pltpu.make_async_remote_copy(
            src_ref=src, dst_ref=dst, send_sem=send, recv_sem=recv,
            device_id={"rows": row + dy, "cols": col + dx}, device_id_type=MESH)

    def cols_of(dx, depth):
        if dx > 0:
            return pl.ds(bx - depth, depth), pl.ds(PAD - depth, depth)
        return pl.ds(0, depth), pl.ds(0, depth)

    def rows_of(dy, depth):
        if dy > 0:
            return pl.ds(top + by - depth, depth), pl.ds(top - depth, depth)
        return pl.ds(top, depth), pl.ds(top + by, depth)

    def reach(p, c):
        if c < 0:
            return 0
        return by if c == chunks - 1 else min(by, cuts[c + 1] + STEPS - 1 - p * DEPTH)

    def near_side(first):
        return jnp.where(down, row > 0, row < rows - 1) if first else jnp.where(down, row < rows - 1, row > 0)

    def column_copies(p, c):
        v, n = reach(p, c - 1), reach(p, c) - reach(p, c - 1)
        out = []
        if not n:
            return out
        lines = pl.ds(at(v, n), n)
        for i, dx in enumerate((-1, 1)):
            xs, xd = cols_of(dx, DEPTH - 1)
            mine = [remote(main.at[p * DEPTH, lines, xs], halo.at[p * DEPTH, lines, xd],
                           col_send.at[p, c, i, 0], col_recv.at[p, c, i, 0], 0, dx)]
            if p == 0:
                xs, xd = cols_of(dx, 1)
                mine.append(remote(f.at[:, lines, xs], fh.at[:, lines, xd],
                                   col_send.at[p, c, i, 1], col_recv.at[p, c, i, 1], 0, dx))
            out.append((exists(0, dx), exists(0, -dx), mine))
        return out

    def ahead_copies(p, c):
        v, n = reach(p, c - 1), reach(p, c) - reach(p, c - 1)
        if not n:
            return []
        lines = pl.ds(at(v, n), n)
        out = []
        for i, dx in enumerate((-1, 1)):
            x = pl.ds(1, 1) if dx < 0 else pl.ds(PAD - 2, 1)
            out.append((exists(0, dx), exists(0, -dx), [
                remote(early.at[p, i, lines, x], landed.at[p, lines, x],
                       col_send.at[p, c, i, 2], col_recv.at[p, c, i, 2], 0, dx)]))
        return out

    def edge_copies(p, first):
        e, out = 0 if first else 1, []
        y = pl.ds(at(0 if first else by - 1, 1), 1)
        for i, dx in enumerate((-1, 1)):
            xs, xd = (pl.ds(2, 1),) * 2 if dx < 0 else (pl.ds(bx - 3, 1), pl.ds(PAD - 3, 1))
            mine = [remote(main.at[p * DEPTH, y, xs], halo.at[p * DEPTH, y, xd],
                           edge_send.at[p, e, i, 0], edge_recv.at[p, e, i, 0], 0, dx)]
            if p == 0:
                xs, xd = (pl.ds(1, 1),) * 2 if dx < 0 else (pl.ds(bx - 2, 1), pl.ds(PAD - 2, 1))
                mine.append(remote(f.at[:, y, xs], fh.at[:, y, xd],
                                   edge_send.at[p, e, i, 1], edge_recv.at[p, e, i, 1], 0, dx))
            out.append((jnp.logical_and(near_side(first), exists(0, dx)),
                        jnp.logical_and(near_side(first), exists(0, -dx)), mine))
        return out

    def border_copies(p, first, corners):
        out = []
        for i, dy in enumerate((-1, 1)):
            here = down if (dy < 0) == first else jnp.logical_not(down)
            there = down if (dy > 0) == first else jnp.logical_not(down)
            ys, yd = rows_of(dy, DEPTH)
            mine = [remote(main.at[p * DEPTH, ys], main.at[p * DEPTH, yd],
                           row_send.at[p, i, 0], row_recv.at[p, i, 0], dy, 0)]
            if p == 0:
                ys, yd = rows_of(dy, DEPTH - 1)
                mine.append(remote(f.at[:, ys], f.at[:, yd],
                                   row_send.at[p, i, 1], row_recv.at[p, i, 1], dy, 0))
            if not corners:
                out.append((jnp.logical_and(here, exists(dy, 0)), jnp.logical_and(there, exists(-dy, 0)), mine))
                continue
            for j, dx in enumerate((-1, 1)):
                (ys, yd), (xs, xd) = rows_of(dy, DEPTH - 1), cols_of(dx, DEPTH - 1)
                mine = [remote(main.at[p * DEPTH, ys, xs], halo.at[p * DEPTH, yd, xd],
                               corner_send.at[p, i, j, 0], corner_recv.at[p, i, j, 0], dy, dx)]
                if p == 0 and DEPTH > 2:
                    (ys, yd), (xs, xd) = rows_of(dy, DEPTH - 2), cols_of(dx, DEPTH - 2)
                    mine.append(remote(f.at[:, ys, xs], fh.at[:, yd, xd],
                                       corner_send.at[p, i, j, 1], corner_recv.at[p, i, j, 1], dy, dx))
                out.append((jnp.logical_and(here, exists(dy, dx)),
                            jnp.logical_and(there, exists(-dy, -dx)), mine))
        return out

    def corner_copies(p, c):
        out = []
        if c == 0 and rows > 2:
            out = border_copies(p, True, True) + edge_copies(p, True)
        if c == chunks - 1:
            out = out + border_copies(p, False, True) + edge_copies(p, False)
        return out

    def side_copies(p, c):
        out = column_copies(p, c)
        if c == 0 and rows > 2:
            out = out + border_copies(p, True, False)
        if c == chunks - 1:
            out = out + border_copies(p, False, False)
        return out

    def exchange(p, c):
        return corner_copies(p, c) + side_copies(p, c) + ahead_copies(p, c)

    def start(jobs):
        for here, _, copies in jobs:
            @pl.when(here)
            def _():
                for copy in copies:
                    copy.start()

    def finish(jobs):
        for _, there, copies in jobs:
            @pl.when(there)
            def _():
                for copy in copies:
                    copy.wait_recv()

    def drain(jobs):
        for here, _, copies in jobs:
            @pl.when(here)
            def _():
                for copy in copies:
                    copy.wait_send()

    column = lax.broadcasted_iota(jnp.int32, (1, PAD, 128), 1)
    keep = jnp.logical_and(
        jnp.logical_or(column < HALF, jnp.broadcast_to(col > 0, column.shape)),
        jnp.logical_or(column >= HALF, jnp.broadcast_to(col < cols - 1, column.shape)))

    def mix(c, above, below, right, left, fy, fx):
        spread = (above + below) + (right + left)
        return (0.8 * c + 0.05 * spread) - fy * (above - below) - fx * (right - left)

    def new_main(s, y, k, beyond=False):
        c = main[s, pl.ds(y, k)]
        wide = jnp.concatenate([c, halo[s, pl.ds(y, k)]], axis=1)
        right, left = pltpu.roll(wide, bx + PAD - 1, 1)[:, :bx], pltpu.roll(wide, 1, 1)[:, :bx]
        above, below = main[s, pl.ds(y + 1, k)], main[s, pl.ds(y - 1, k)]
        if beyond:
            return mix(c, above, below, right, left, f[0, pl.ds(y, k)], f[1, pl.ds(y, k)])
        up, down, ahead, back = (weight[i, pl.ds(y - top, k)] for i in range(4))
        return ((0.8 * c + up * above) + down * below) + (ahead * right + back * left)

    def new_halo(s, y, k):
        c = halo[s, pl.ds(y, k)]
        wide = jnp.concatenate([main[s, pl.ds(y, k), pl.ds(bx - PAD, PAD)], c,
                                main[s, pl.ds(y, k), pl.ds(0, PAD)]], axis=1)
        right = pltpu.roll(wide, 3 * PAD - 1, 1)[:, PAD:2 * PAD]
        left = pltpu.roll(wide, 1, 1)[:, PAD:2 * PAD]
        new = mix(c, halo[s, pl.ds(y + 1, k)], halo[s, pl.ds(y - 1, k)], right, left,
                  fh[0, pl.ds(y, k)], fh[1, pl.ds(y, k)])
        return jnp.where(keep, new, 0.0)

    ahead_column = jnp.logical_or(column == 1, column == PAD - 2)

    def take_ahead(p, v, n):
        def do(y, k, always=True):
            got = ahead_column if always is True else jnp.logical_and(ahead_column, always)
            new = jnp.where(got, landed[p, pl.ds(y, k)], new_halo(p * DEPTH, y, k))
            halo[p * DEPTH + 1, pl.ds(y, k)] = jnp.where(keep, new, 0.0)
        end = v + n
        if v == 0 and rows > 2:
            v = 1
            do(at(0, 1), 1, jnp.broadcast_to(jnp.logical_not(near_side(True)), column.shape))
        if end == by:
            end = by - 1
            do(at(by - 1, 1), 1, jnp.broadcast_to(jnp.logical_not(near_side(False)), column.shape))
        over(v, end - v, 16, do)

    def send_ahead(p, c):
        v, n = reach(p, c - 1), reach(p, c) - reach(p, c - 1)

        def do(y, k):
            for i, x in enumerate((pl.ds(0, PAD), pl.ds(bx - PAD, PAD))):
                tile = main[p * DEPTH, pl.ds(y, k), x]
                early[p, i, pl.ds(y, k)] = mix(
                    tile, main[p * DEPTH, pl.ds(y + 1, k), x], main[p * DEPTH, pl.ds(y - 1, k), x],
                    pltpu.roll(tile, PAD - 1, 1), pltpu.roll(tile, 1, 1),
                    f[0, pl.ds(y, k), x], f[1, pl.ds(y, k), x])
        end = v + n
        if v == 0 and rows > 2:
            v = 1

            @pl.when(jnp.logical_not(near_side(True)))
            def _():
                do(at(0, 1), 1)
        if end == by:
            end = by - 1

            @pl.when(jnp.logical_not(near_side(False)))
            def _():
                do(at(by - 1, 1), 1)
        over(v, end - v, 8, do)

    def over(v, n, k, do):
        if n <= 0:
            return
        y = at(v, n)
        whole = n // k
        if whole > 1:
            @pl.loop(0, whole)
            def _(i):
                do(y + i * k, k)
        elif whole:
            do(y, k)
        if n % k:
            do(y + whole * k, n % k)

    def write_main(s, beyond=False):
        def do(y, k):
            main[s, pl.ds(y, k)] = new_main(s - 1, y, k, beyond)
        return do

    def write_edges(s):
        def do(y, k):
            lines = pl.ds(y, k)
            for x, wide in (
                (0, (halo[s - 1, lines], main[s - 1, lines, pl.ds(0, 2 * PAD)])),
                (bx - PAD, (main[s - 1, lines, pl.ds(bx - 2 * PAD, 2 * PAD)], halo[s - 1, lines])),
            ):
                tile = pl.ds(x, PAD)
                wide = jnp.concatenate(wide, axis=1)
                right = pltpu.roll(wide, 3 * PAD - 1, 1)[:, PAD:2 * PAD]
                left = pltpu.roll(wide, 1, 1)[:, PAD:2 * PAD]
                up, down, front, back = (weight[i, pl.ds(y - top, k), tile] for i in range(4))
                main[s, lines, tile] = (
                    (0.8 * wide[:, PAD:2 * PAD] + up * main[s - 1, pl.ds(y + 1, k), tile])
                    + down * main[s - 1, pl.ds(y - 1, k), tile]
                ) + (front * right + back * left)
        return do

    def settle(p):
        def step(s):
            def do(y, k):
                c = main[s - 1, pl.ds(y, k)]
                up, down, front, back = (weight[i, pl.ds(y - top, k)] for i in range(4))
                main[s, pl.ds(y, k)] = (
                    (0.8 * c + up * main[s - 1, pl.ds(y + 1, k)]) + down * main[s - 1, pl.ds(y - 1, k)]
                ) + (front * pltpu.roll(c, bx - 1, 1) + back * pltpu.roll(c, 1, 1))
            return do
        for i in range(1, DEPTH + 1):
            s = p * DEPTH + i
            if s < STEPS:
                low = i if rows > 2 else 0
                over(low, by - i - low, 8, step(s))

    def write_halo(s):
        def do(y, k):
            halo[s, pl.ds(y, k)] = new_halo(s - 1, y, k)
        return do

    def advance(p, c):
        cuts = plan[p]
        chunks = len(cuts) - 1
        for i in range(1, DEPTH + 1):
            s = p * DEPTH + i
            ahead = STEPS - s
            low = 0 if c == 0 else min(by, cuts[c] + ahead)
            high = by if c == chunks - 1 else min(by, cuts[c + 1] + ahead)
            if s == STEPS:
                break
            start_v = max(low, DEPTH if rows > 2 else 0)
            end_v = min(high, by - DEPTH)
            over(low, start_v - low, 8, write_main(s))
            over(start_v, end_v - start_v, 8, write_edges(s))
            over(end_v, high - end_v, 8, write_main(s))
            if i < DEPTH:
                low = low - 1 if c else 0
                high = high if c == chunks - 1 else high - 1
                if i == 1:
                    take_ahead(p, low, high - low)
                else:
                    over(low, high - low, 16, write_halo(s))
                margin = DEPTH - i
                for first in (True, False):
                    if c != (0 if first else chunks - 1) or first and rows <= 2:
                        continue
                    for dy in (-1, 1):
                        here = down if (dy < 0) == first else jnp.logical_not(down)

                        @pl.when(jnp.logical_and(here, exists(dy, 0)))
                        def _():
                            y = top - margin if dy < 0 else top + by
                            write_main(s, True)(y, margin)
                            write_halo(s)(y, margin)
        return low, high

    pieces = len(fine) - 1

    def share(c, to, sender):
        if c < pieces:
            n = fine[c + 1] - fine[c]
            lines = pl.ds(pl.multiple_of(at(fine[c], n) - top, 8), n)
        else:
            lines = pl.ds(0, by)
        return pltpu.make_async_remote_copy(
            src_ref=stats.at[:, lines], dst_ref=gathered.at[sender, :, lines],
            send_sem=stat_send.at[c, to], recv_sem=stat_recv.at[c, sender],
            device_id={"cols": to}, device_id_type=MESH)

    def each_peer(low, high, do):
        if high - low <= 8:
            for k in range(low, high):
                @pl.when(col != k)
                def _():
                    do(k)
        else:
            @pl.loop(low, high)
            def _(k):
                @pl.when(col != k)
                def _():
                    do(k)

    head = min(HEAD, cols) if pieces > 1 else 0

    def last_step(v, n):
        y = at(v, n)

        @pl.loop(0, n // 8)
        def _(i):
            new = new_main(STEPS - 1, y + i * 8, 8)
            out = pl.ds(pl.multiple_of(y - top + i * 8, 8), 8)
            final[out] = new
            mean = jnp.sum(new, axis=1) / bx
            off = new - mean[:, None, :]
            second = jnp.sum(off * off, axis=1)
            stats[0, out] = mean
            stats[1, out] = second
            gathered[col, 0, out] = mean
            gathered[col, 1, out] = second

    def combine(c):
        n = fine[c + 1] - fine[c]
        y = at(fine[c], n) - top

        @pl.loop(0, n // 8)
        def _(i):
            lines = pl.ds(pl.multiple_of(y + i * 8, 8), 8)
            means = [gathered[k, 0, lines] for k in range(cols)]
            mean = sum(means[1:], means[0]) / cols
            parts = [gathered[k, 1, lines] + bx * ((means[k] - mean) * (means[k] - mean)) for k in range(cols)]
            spread = sum(parts[1:], parts[0])
            moments[0, lines] = mean
            moments[1, lines] = lax.rsqrt(spread / (bx * cols) + 0.0001)

    pl.semaphore_wait(barrier, across + upright)
    for dy in (-1, 1):
        @pl.when(exists(dy, 0))
        def _():
            pl.semaphore_signal(heard, inc=1, device_id={"rows": row + dy}, device_id_type=MESH)
    send_token(0)
    for load in loads:
        load.wait()
    for c in range(chunks):
        start(side_copies(0, c))
        send_ahead(0, c)
        start(ahead_copies(0, c))
    @pl.loop(0, by // 4)
    def _(i):
        lines = pl.ds(i * 4, 4)
        for d in range(2):
            flow = f[d, pl.ds(top + i * 4, 4)]
            weight[2 * d, lines] = 0.05 - flow
            weight[2 * d + 1, lines] = 0.05 + flow

    known = 0

    def learn():
        take_token(known)
        send_token(known + 1)
        return known + 1

    pl.semaphore_wait(heard, upright)
    for c in range(chunks):
        start(corner_copies(0, c))
    while known < len(spread_to) - 1:
        known = learn()
    for p in range(PHASES):
        taken = 0
        settle(p)
        for c in range(len(plan[p]) - 1):
            while taken < chunks and cuts[taken] < plan[p][c + 1]:
                finish(exchange(p, taken))
                taken += 1
            low, high = advance(p, c)
            if p + 1 < PHASES:
                start(corner_copies(p + 1, c))
                start(side_copies(p + 1, c))
                send_ahead(p + 1, c)
                start(ahead_copies(p + 1, c))
            else:
                last_step(low, high - low)
                while known < len(spread_to):
                    known = learn()
                if head:
                    each_peer(0, head, lambda k: share(c, k, col).start())
    def later(k):
        @pl.when(k > col)
        def _():
            share(pieces, k, col).start()

    def earlier(k):
        @pl.when(k < col)
        def _():
            share(pieces, k, col).start()
    each_peer(head, cols, later)

    @pl.when(jnp.logical_and(col > head, col < cols - 2))
    def _():
        pl.delay(HOLD[0])

    @pl.when(jnp.logical_and(col > head, col >= cols - 2))
    def _():
        pl.delay(HOLD[1])
    each_peer(head, cols, earlier)
    if head:
        @pl.when(col < head)
        def _():
            for c in range(pieces):
                each_peer(0, cols, lambda k: share(c, k, k).wait_recv())
                combine(c)

        @pl.when(col >= head)
        def _():
            each_peer(0, cols, lambda k: share(pieces, k, k).wait_recv())
            for c in range(pieces):
                combine(c)
    else:
        each_peer(0, cols, lambda k: share(pieces, k, k).wait_recv())
        for c in range(pieces):
            combine(c)
    for c in range(chunks):
        for p in range(PHASES):
            drain(exchange(p, c))
    for c in range(pieces):
        if head:
            each_peer(0, head, lambda k: share(c, k, col).wait_send())
    each_peer(head, cols, lambda k: share(pieces, k, col).wait_send())


def scale_kernel(end, lines, scaled_out, end_out, scaled, sem):
    parts = 4
    g = end.shape[0] // parts
    whole = pltpu.make_async_copy(end, end_out, sem.at[parts])
    stores = [whole]
    for i in range(parts):
        part = pl.ds(i * g, g)
        scaled[part] = (end[part] - lines[0, part][:, None, :]) * lines[1, part][:, None, :]
        store = pltpu.make_async_copy(scaled.at[part], scaled_out.at[part], sem.at[i])
        store.start()
        stores.append(store)
        if i == 0:
            whole.start()
    for store in stores:
        store.wait()


def shards(rows, cols, tracer, flow_y, flow_x):
    by, bx, species = tracer.shape
    cuts, fine = ((0,) + tuple(cut for cut in chosen if cut < by) + (by,) for chosen in (CUTS, FINE))
    chunks = len(cuts) - 1
    pieces = len(fine) - 1
    tall = by + 2 * DEPTH
    block = jax.ShapeDtypeStruct(tracer.shape, jnp.float32)
    hbm = pl.BlockSpec(memory_space=pl.ANY)
    dma = pltpu.SemaphoreType.DMA
    end, lines = pl.pallas_call(
        functools.partial(kernel, rows, cols, by, bx, cuts, fine),
        out_shape=(pltpu.VMEM(tracer.shape, jnp.float32), pltpu.VMEM((2, by, species), jnp.float32)),
        in_specs=[pl.BlockSpec(memory_space=pltpu.HBM)] * 3,
        out_specs=(pl.BlockSpec(memory_space=pltpu.VMEM),) * 2,
        scratch_shapes=[
            pltpu.VMEM((STEPS, tall, bx, species), jnp.float32),
            pltpu.VMEM((STEPS, tall, PAD, species), jnp.float32),
            pltpu.VMEM((2, tall, bx, species), jnp.float32),
            pltpu.VMEM((2, tall, PAD, species), jnp.float32),
            pltpu.VMEM((4, by, bx, species), jnp.float32),
            pltpu.VMEM((PHASES, 2, tall, PAD, species), jnp.float32),
            pltpu.VMEM((PHASES, tall, PAD, species), jnp.float32),
            pltpu.VMEM((2, by, species), jnp.float32),
            pltpu.VMEM((cols, 2, by, species), jnp.float32),
            dma((3,)),
            dma((PHASES, chunks, 2, 3)), dma((PHASES, chunks, 2, 3)),
            dma((PHASES, 2, 2)), dma((PHASES, 2, 2)),
            dma((PHASES, 2, 2, 2)), dma((PHASES, 2, 2, 2)),
            dma((PHASES, 2, 2, 2)), dma((PHASES, 2, 2, 2)),
            dma((pieces + 1, cols)), dma((pieces + 1, cols)),
            pltpu.SemaphoreType.REGULAR((max(1, len(radii(cols))),)),
            pltpu.SemaphoreType.REGULAR,
        ],
        compiler_params=pltpu.CompilerParams(
            collective_id=0, has_side_effects=True, vmem_limit_bytes=67043328 - 1024 * 1024),
    )(tracer, flow_y, flow_x)
    return pl.pallas_call(
        scale_kernel,
        out_shape=(block, block),
        in_specs=[pl.BlockSpec(memory_space=pltpu.VMEM)] * 2,
        out_specs=(hbm, hbm),
        scratch_shapes=[
            pltpu.VMEM(tracer.shape, jnp.float32),
            pltpu.SemaphoreType.DMA((5,)),
        ],
        compiler_params=pltpu.CompilerParams(vmem_limit_bytes=40 * 1024 * 1024),
    )(end, lines)


def solution(mesh):
    placed = P(("site", "rows"), "cols", None)
    return jax.shard_map(
        functools.partial(shards, mesh.shape["rows"], mesh.shape["cols"]),
        mesh=mesh,
        in_specs=(placed,) * 3,
        out_specs=(placed, placed),
        check_vma=False,
    )
```
